512 devices in a mesh: row: 16 (over x, y_lo, core), col: 32 (over z, y_hi).
Axes of the slice: x: 4, y: 8 (y_hi: 4, y_lo: 2; y = y_hi * 2 + y_lo), z: 8, core: 2. Of those that a mesh axis runs over, the one named last changes fastest.
Arguments:
- item_ids: int32 [131072], P(('row', 'col')), may hold values from 0 to 1023
- user_lengths: int32 [32], replicated, may hold values from 1 to 8192, 131072 in all
- catalogue: bfloat16 [1024, 1024], P(('row', 'col')), may hold values from -6 to 6
- tap_lengths: int32 [1, 1024], replicated, may hold values from 64 to 256
- conv_taps: bfloat16 [1, 256, 1024], replicated, may hold values from -0.375 to 0.375
- norm_gains: float32 [1, 2, 1024], replicated, may hold values from 0.1 to 1.9
- gate_weight: bfloat16 [1, 1024, 1024], P(None, 'col'), may hold values from -0.1875 to 0.1875
- up_weight: bfloat16 [1, 1024, 1024], P(None, 'col'), may hold values from -0.1875 to 0.1875
- down_weight: bfloat16 [1, 1024, 1024], P(None, 'col'), may hold values from -0.1875 to 0.1875
Outputs:
- history_out: bfloat16 [131072, 1024], P(('row', 'col'))
The draws below stay inside these ranges and needn't reach their ends.
Inputs may be any that keep to these rules, and one draw needn't show every extreme that they name: `user_lengths`: the 32 lengths sum to 131072.
All inputs are finite; a program needn't handle non-finite values.
Results may differ from the reference program's by a relative error of at most 0.0054.
Values may be sent and summed in bfloat16 or wider, within the bound.
A program may use at most 64 MiB of HBM per device.

```python
import math
import jax
import jax.numpy as jnp
import numpy as np
from jax import lax

D = 1024
FF = 1024
K = 256
LAYERS = 1
TOK_DEV = 256
TOKENS = 131072
ITEMS = 1024
USERS = 32
N_ROW = 16


def set_ends(entries, own_key, least, largest):
    longest = entries.shape.index(max(entries.shape))
    spots = []
    for shift in (0, 1):
        where = [jax.random.randint(jax.random.fold_in(own_key, axis), (), 0, length) for axis, length in enumerate(entries.shape)]
        where[longest] = (where[longest] + shift) % entries.shape[longest]
        spots.append(tuple(where))
    return entries.at[spots[0]].set(least).at[spots[1]].set(largest)


def steps_of(own_key, extent, shards, least, largest):
    gain = 1.0
    for position, blocks in shards:
        steps = jax.random.uniform(jax.random.fold_in(jax.random.fold_in(own_key, 6), position), (blocks,), jnp.float32, least / len(shards), largest / len(shards))
        gain = gain * jnp.repeat(jnp.exp(steps), extent[position] // blocks).reshape((-1,) + (1,) * (len(extent) - 1 - position))
    return gain


def cumulative_ranks(count, slope):
    loads = [(1 << 20) // math.isqrt(grade ** slope) + 1 for grade in range(1, count + 1)]
    deviation = 1 + sum(loads) // (1 << 30)
    return np.cumsum(np.array([max(1, weight // deviation) for weight in loads]))


def ranked_ids(key, dims, number_of, slope):
    grid = cumulative_ranks(number_of, slope)
    ticket = jax.random.randint(jax.random.fold_in(key, 1), dims, 0, int(grid[number_of - 1]))
    standing = jnp.searchsorted(jnp.asarray(grid, jnp.int32), ticket, side="right")
    return jax.random.permutation(jax.random.fold_in(key, 2), number_of)[standing].astype(jnp.int32)


def profile(amount, total, bound, lean):
    loads = [(1 << 20) // math.isqrt(grade ** lean) + 1 for grade in range(2, amount + 1)]
    spare, counts = total - bound - (amount - 1), [1] * (amount - 1)
    while spare > 0:
        movable = [i for i in range(amount - 1) if counts[i] < bound]
        whole, left = sum([loads[i] for i in movable]), spare
        for i in movable:
            more = min(bound - counts[i], max(1, left * loads[i] // whole), spare)
            counts[i] = counts[i] + more
            spare = spare - more
    return np.array([bound] + counts)


def ragged_sizes(own_key, amount, total, reach, slope):
    if amount == 2:
        one = jax.random.randint(own_key, (), max(1, total - reach), min(reach, total - 1) + 1)
        return jnp.stack([one, total - one])
    lengths = jnp.asarray(profile(amount, total, reach, slope), jnp.int32)
    twos = (amount - 1) // 2
    source_of, sink = lengths[1:1 + 2 * twos:2], lengths[2:2 + 2 * twos:2]
    slack = jnp.minimum(source_of - 1, reach - sink)
    passed = jax.random.randint(jax.random.fold_in(own_key, 1), (twos,), 0, 1 << 20) % (slack + 1)
    lengths = lengths.at[1:1 + 2 * twos:2].set(source_of - passed).at[2:2 + 2 * twos:2].set(sink + passed)
    return lengths[jax.random.permutation(jax.random.fold_in(own_key, 2), amount)]


def normal_values(key, shape, spread, bound, shards=(), kind=jnp.bfloat16):
    entries = spread * jax.random.normal(key, shape, jnp.float32)
    if shards:
        entries = entries * steps_of(key, shape, shards, -0.22, 0.18)
    return jnp.clip(entries, -bound, bound).astype(kind)


def setup_inputs(seed: int = 0) -> dict:
    key_list = jax.random.split(jax.random.key(seed), 10)
    item_ids = set_ends(ranked_ids(key_list[0], (TOKENS,), ITEMS, 2), jax.random.fold_in(key_list[0], 3), 0, ITEMS - 1).astype(jnp.int32)
    user_lengths = ragged_sizes(key_list[1], USERS, TOKENS, TOKENS // N_ROW, 2).astype(jnp.int32)
    catalogue = normal_values(key_list[2], (ITEMS, D), 1.0, 6.0, ((0, 512),))
    tap_lengths = set_ends(jax.random.randint(key_list[3], (LAYERS, D), K // 4, K + 1), jax.random.fold_in(key_list[3], 1), K // 4, K).astype(jnp.int32)
    conv_taps = normal_values(key_list[4], (LAYERS, K, D), K ** -0.5, 0.375)
    norm_gains = jnp.clip(1.0 + 0.18 * jax.random.normal(key_list[5], (LAYERS, 2, D), jnp.float32), 0.1, 1.9)
    gate_weight = normal_values(key_list[6], (LAYERS, D, FF), D ** -0.5, 0.1875, ((1, 32),))
    up_weight = normal_values(key_list[7], (LAYERS, D, FF), D ** -0.5, 0.1875, ((1, 32),))
    down_weight = normal_values(key_list[8], (LAYERS, FF, D), FF ** -0.5, 0.1875, ((1, 32),))
    return dict(item_ids=item_ids, user_lengths=user_lengths, catalogue=catalogue, tap_lengths=tap_lengths, conv_taps=conv_taps, norm_gains=norm_gains, gate_weight=gate_weight, up_weight=up_weight, down_weight=down_weight)


epsilon = 1e-06

def rms_norm(values, gains):
    scale = lax.rsqrt(lax.optimization_barrier(jnp.mean(values * values, axis=-1, keepdims=True)) + epsilon)
    return values * scale * gains

def token_ages(positions, user_starts):
    reached = user_starts[None, :] <= positions[:, None]
    fallback = jnp.minimum(positions, 0)[:, None]
    seg_start = lax.optimization_barrier(jnp.max(jnp.where(reached, user_starts[None, :], fallback), axis=1))
    return positions - seg_start

def reference(item_ids, user_lengths, catalogue, tap_lengths, conv_taps, norm_gains, gate_weight, up_weight, down_weight):
    hidden = jnp.take(catalogue, item_ids, axis=0).astype(jnp.float32)
    positions = jnp.arange(TOKENS, dtype=jnp.int32)
    user_starts = (jnp.cumsum(user_lengths) - user_lengths).astype(jnp.int32)
    token_age = token_ages(positions, user_starts)
    lag_column = jnp.arange(K, dtype=jnp.int32)[:, None]
    block_count = TOKENS // TOK_DEV
    for layer_index in range(LAYERS):
        normed = rms_norm(hidden, norm_gains[layer_index, 0]).astype(jnp.bfloat16)
        tap_table = conv_taps[layer_index].astype(jnp.float32) * (lag_column < tap_lengths[layer_index][None, :]).astype(jnp.float32)
        padded = jnp.concatenate([jnp.zeros((K - 1, D), jnp.bfloat16), normed], axis=0)
        gains_inner = norm_gains[layer_index, 1]
        gate_now = gate_weight[layer_index]
        up_now = up_weight[layer_index]
        down_now = down_weight[layer_index]

        def one_block(block_index):
            start = (block_index * TOK_DEV).astype(jnp.int32)
            extended = lax.dynamic_slice_in_dim(padded, start, TOK_DEV + K - 1, 0)
            ages = lax.dynamic_slice_in_dim(token_age, start, TOK_DEV, 0)
            rows = lax.dynamic_slice_in_dim(hidden, start, TOK_DEV, 0)

            def add_lag(lag_index, accumulated):
                begin = (K - 1 - lag_index).astype(jnp.int32)
                shifted = lax.dynamic_slice_in_dim(extended, begin, TOK_DEV, 0)
                weights = lax.dynamic_slice_in_dim(tap_table, jnp.asarray(lag_index).astype(jnp.int32), 1, 0)
                keep = (lag_index <= ages)[:, None]
                return accumulated + jnp.where(keep, shifted.astype(jnp.float32) * weights, 0.0)
            mixing = lax.fori_loop(0, K, add_lag, jnp.zeros((TOK_DEV, D), jnp.float32))
            rows = rows + mixing
            inner = rms_norm(rows, gains_inner).astype(jnp.bfloat16)
            gate_sum = jnp.dot(inner, gate_now, preferred_element_type=jnp.float32)
            up_sum = jnp.dot(inner, up_now, preferred_element_type=jnp.float32)
            activated = (jax.nn.silu(gate_sum) * up_sum).astype(jnp.bfloat16)
            return rows + jnp.dot(activated, down_now, preferred_element_type=jnp.float32)
        blocks = lax.map(one_block, jnp.arange(block_count, dtype=jnp.int32))
        hidden = blocks.reshape(TOKENS, D)
    return hidden.astype(jnp.bfloat16)
```

```python
import functools
import jax
import jax.numpy as jnp
from jax import lax
from jax.experimental import pallas as pl
from jax.experimental.pallas import tpu as pltpu
from jax.sharding import Mesh
from jax.sharding import PartitionSpec as P

BF = jnp.bfloat16
F32 = jnp.float32
EPS = 1e-6
MESH = pl.DeviceIdType.MESH


SIZES = (("x", 4), ("yl", 2), ("c", 2), ("z", 8), ("yh", 4))
N_SEM = 224


class Net:
    def __init__(self, send, recv):
        self.send_sem, self.recv_sem, self.used, self.open = send, recv, 0, []
        self.at = {n: lax.axis_index(n) for n, _ in SIZES}

    def peer(self, **other):
        return {n: other.get(n, self.at[n]) for n, _ in SIZES}

    def step(self, distance):
        flat = jnp.int32(0)
        for n, size in SIZES:
            flat = flat * size + self.at[n]
        flat = lax.rem(flat + distance + 512, 512)
        out = {}
        for n, size in reversed(SIZES):
            out[n] = lax.rem(flat, size)
            flat = flat // size
        return out

    def copy(self, src, dst, to):
        k = self.used
        self.used += 1
        one = pltpu.make_async_remote_copy(
            src_ref=src, dst_ref=dst, send_sem=self.send_sem.at[k], recv_sem=self.recv_sem.at[k],
            device_id=to, device_id_type=MESH)
        one.start()
        self.open.append(one)
        return one

    def finish(self):
        for one in self.open:
            one.wait_send()


def geometry(net):
    a = net.at
    d = 2 * a["yl"] - 1
    e = 2 * lax.rem(a["z"], 2) - 1
    g = {}
    g["d"], g["e"] = d, e
    g["y_far"] = net.peer(yh=lax.rem(a["yh"] + d + 4, 4), yl=1 - a["yl"])
    g["y_near"] = net.peer(yl=1 - a["yl"])
    g["z_far"] = net.peer(z=lax.rem(a["z"] + e + 8, 8))
    g["z_near"] = net.peer(z=lax.rem(a["z"] - e + 8, 8))
    g["z_up"] = net.peer(z=lax.rem(a["z"] + 1, 8))
    g["z_down"] = net.peer(z=lax.rem(a["z"] + 7, 8))
    g["twin"] = net.peer(c=1 - a["c"])
    g["xs"] = [net.peer(x=lax.rem(a["x"] + s, 4)) for s in (1, 3, 2)]
    zh = a["z"] // 2
    g["zh"] = zh
    g["group"] = []
    for dc in range(2):
        for dz in range(2):
            for dy in range(4):
                if dc or dz or dy:
                    g["group"].append(net.peer(
                        c=lax.rem(a["c"] + dc, 2), z=2 * zh + lax.rem(a["z"] + dz, 2), yh=lax.rem(a["yh"] + dy, 4)))
    g["next"], g["prev"] = net.step(1), net.step(-1)
    return g


def entry(g):
    barrier = pltpu.get_barrier_semaphore()
    near = g["group"] + g["xs"] + [g["y_far"], g["y_near"], g["z_far"], g["z_near"], g["next"], g["prev"]]
    for to in near:
        pl.semaphore_signal(barrier, inc=1, device_id=to, device_id_type=MESH)
    pl.semaphore_wait(barrier, len(near))


def pair_ring(block, h, d, count, far, near, net):
    one = net.copy(block(h, True), block(h, False), far)
    yield
    one.wait_recv()
    key = lax.rem(h + d + count, count)
    net.share(block(key, False))
    one = net.copy(block(key, False), block(key, False), near)
    yield
    one.wait_recv()
    key = lax.rem(h - d + count, count)
    net.share(block(key, False))
    one = net.copy(block(key, False), block(key, False), far)
    yield
    one.wait_recv()
    net.share(block(lax.rem(h + 2, count), False))


def ring_of_8(block, z, c, up, down, net):
    a = net.copy(block(z, True), block(z, False), up)
    b = net.copy(block(z, True), block(z, False), down)
    yield
    for hop in (1, 2):
        a.wait_recv()
        key = lax.rem(z - hop + 8, 8)
        net.share(block(key, False))
        a = net.copy(block(key, False), block(key, False), up)
        b.wait_recv()
        key = lax.rem(z + hop, 8)
        net.share(block(key, False))
        b = net.copy(block(key, False), block(key, False), down)
        yield
    a.wait_recv()
    net.share(block(lax.rem(z - 3 + 8, 8), False))
    b.wait_recv()
    net.share(block(lax.rem(z + 3, 8), False))
    key = lax.rem(z - 3 + 6 * c + 8, 8)
    to = {n: jnp.where(c == 0, up[n], down[n]) for n in up}
    a = net.copy(block(key, False), block(key, False), to)
    yield
    a.wait_recv()
    net.share(block(lax.rem(z + 4, 8), False))


def gather_kernel(ids_ref, cat_ref, gate_ref, up_ref, down_ref, ids_out, catb, wb, pairs, fill_sem, send, recv):
    net = Net(send, recv)
    g = geometry(net)
    shared = []
    net.share = lambda ref: shared.append(net.copy(ref, ref, g["twin"]))
    a = net.at
    x, yl, c, z, yh, zh = a["x"], a["yl"], a["c"], a["z"], a["yh"], g["zh"]
    fill = []
    for n, ref in enumerate((gate_ref, up_ref, down_ref)):
        for t in range(8):
            one = pltpu.make_async_copy(ref.at[:, 128 * t:128 * t + 128], wb.at[t, n, z, yh], fill_sem.at[8 * n + t])
            one.start()
            fill.append(one)
    entry(g)

    lanes = pl.ds(4 * c, 4)

    def w_y_first(t):
        lt = 4 * c + t
        yield from pair_ring(lambda h, _: wb.at[lt, :, z, h], yh, g["d"], 4, g["y_far"], g["y_near"], net)
        yield from ring_of_8(lambda k, _: wb.at[lt, :, k], z, c, g["z_up"], g["z_down"], net)

    def w_z_first(t):
        lt = 4 * c + t
        yield from ring_of_8(lambda k, _: wb.at[lt, :, k, yh], z, c, g["z_up"], g["z_down"], net)
        yield from pair_ring(lambda h, _: wb.at[lt, :, :, h], yh, g["d"], 4, g["y_far"], g["y_near"], net)

    def cat_x():
        net.share(catb.at[lanes, x, yl, :, zh])
        ref = catb.at[lanes, x, yl, :, zh]
        out = [net.copy(ref, ref, to) for to in g["xs"]]
        yield
        for one, s in zip(out, (1, 3, 2)):
            one.wait_recv()
            net.share(catb.at[lanes, lax.rem(x - s + 4, 4), yl, :, zh])

    def swap_y(part, span):
        send_far = pl.ds(0, 2)
        send_near = pl.ds(2, 2)
        one = net.copy(part(send_far, yl, span), part(send_far, yl, span), g["y_far"])
        two = net.copy(part(send_near, yl, span), part(send_near, yl, span), g["y_near"])
        yield
        one.wait_recv()
        two.wait_recv()
        net.share(part(pl.ds(0, 4), 1 - yl, span))

    def cat_y_first():
        la = pl.ds(4 * c, 2)
        yield from swap_y(lambda xs, k, s: catb.at[la, xs, k, :, s], zh)
        yield from pair_ring(lambda h, _: catb.at[la, :, :, :, h], zh, g["e"], 4, g["z_far"], g["z_near"], net)

    def cat_z_first():
        la = pl.ds(4 * c + 2, 2)
        yield from pair_ring(lambda h, _: catb.at[la, :, yl, :, h], zh, g["e"], 4, g["z_far"], g["z_near"], net)
        yield from swap_y(lambda xs, k, s: catb.at[la, xs, k], None)

    mine = 4 * lax.rem(z, 2) + yh
    group = []
    for to in g["group"]:
        half = pl.ds(pl.multiple_of(512 * to["c"], 512), 512)
        group.append(net.copy(cat_ref.at[:, half], pairs.at[c, mine], to))
    ids = net.copy(ids_ref, ids_out.at[0], g["next"])
    ids_out[1] = ids_ref[...]
    pairs[c, mine] = jnp.where(c == 0, cat_ref[:, 0:512], cat_ref[:, 512:1024])
    for one in fill:
        one.wait()
    weights = [w_y_first(0), w_z_first(2), w_y_first(1), w_z_first(3)]
    for f in weights:
        next(f)
    for one in group:
        one.wait_recv()
    for k in range(2):
        rows = jnp.concatenate([pairs[k, i].astype(F32) for i in range(8)], axis=0).astype(BF)
        for t in range(4):
            catb[4 * c + t, x, yl, k, zh] = rows[:, 128 * t:128 * t + 128]
    def run(flow):
        for _ in flow:
            pass

    run(cat_x())
    flows = [cat_y_first(), cat_z_first()] + weights
    while flows:
        for f in list(flows):
            try:
                next(f)
            except StopIteration:
                flows.remove(f)
    ids.wait_recv()
    for one in shared:
        one.wait_recv()
    net.finish()


def gather(ids, cat, gate, up, down):
    vm = pl.BlockSpec(memory_space=pltpu.VMEM)
    return pl.pallas_call(
        gather_kernel,
        out_shape=(jax.ShapeDtypeStruct((2, 1, 256), jnp.int32),
                   jax.ShapeDtypeStruct((8, 4, 2, 2, 4, 16, 128), BF),
                   jax.ShapeDtypeStruct((8, 3, 8, 4, 32, 128), BF)),
        in_specs=[vm] * 2 + [pl.BlockSpec(memory_space=pl.ANY)] * 3,
        out_specs=(vm,) * 3,
        scratch_shapes=[pltpu.VMEM((2, 8, 2, 512), BF), pltpu.SemaphoreType.DMA((24,)),
                        pltpu.SemaphoreType.DMA((N_SEM,)), pltpu.SemaphoreType.DMA((N_SEM,))],
        compiler_params=pltpu.CompilerParams(collective_id=0, has_side_effects=True, vmem_limit_bytes=40 * 2**20),
    )(ids, cat, gate, up, down)


NT = (((1,), (1,)), ((), ()))


def dot(a, b):
    return jnp.dot(a, b, preferred_element_type=F32)


def dot_nt(a, b):
    return lax.dot_general(a, b, NT, preferred_element_type=F32)


def iota(shape, dim):
    return lax.broadcasted_iota(jnp.int32, shape, dim)


def one(cond):
    return jnp.where(cond, 1.0, 0.0).astype(BF)


def prepare_taps(tl_ref, taps_ref, hr, ht, h):
    p, k = iota((256, 256), 0), iota((256, 256), 1)
    reverse = one(p + k == 256)
    turned = one(k == 16 * (p // 16) + (p % 16 - p // 16 + 16) % 16)
    lag = iota((256, 256), 0)
    for s in range(4):
        cols = slice(256 * s, 256 * s + 256)
        table = jnp.where(lag < tl_ref[:, cols], taps_ref[:, cols].astype(F32), 0.0).astype(BF)
        backward = dot(reverse, table).astype(BF)
        hr[cols, :] = dot_nt(turned, backward).astype(BF)

    def shift_one(j, _):
        shift = one((k == p + j) & (p >= 1))
        for s in range(4):
            rows = dot(hr[256 * s:256 * s + 256, :], shift).astype(BF)
            ht[pl.ds(16 * s, 16), pl.ds(j, 1)] = rows.reshape(16, 1, 16, 256)
        return 0

    lax.fori_loop(0, 16, shift_one, 0)
    unit = one(p == k)

    def flip(g, _):
        for a in range(4):
            h[4 * g + a] = dot_nt(unit, ht[4 * g + a].reshape(256, 256)).astype(BF)
        return 0

    lax.fori_loop(0, 16, flip, 0)


def user_tables(base, len_ref, keep, first, live):
    pos = base + iota((256, 128), 0)
    begin = jnp.zeros((256, 128), jnp.int32)
    pos_b = base + 16 * iota((16, 256), 0)
    begin_b = jnp.zeros((16, 256), jnp.int32)
    start = jnp.int32(0)
    for u in range(len_ref.shape[0]):
        begin = jnp.where(pos >= start, start, begin)
        begin_b = jnp.where(pos_b >= start, start, begin_b)
        start = start + len_ref[u]
    reach = jnp.minimum(pos - begin, iota((256, 128), 0) % 16)
    for lag in range(16):
        keep[lag] = jnp.where(lag <= reach, 1.0, 0.0)
    source = pos_b - 256 + iota((16, 256), 1)
    first[...] = jnp.where(source >= begin_b, 1.0, 0.0)
    head = base + 16 * (iota((256, 128), 0) // 16)
    live[...] = jnp.where(begin < head, 1.0, 0.0)


def wide(ref, n):
    return jnp.concatenate([ref[2 * n], ref[2 * n + 1]], axis=1)


def look_up(ids_ref, cat_ref, gains_ref, hid, nf, nt):
    ids = ids_ref[...].astype(F32)
    for half in range(2):
        row = ids[half:half + 1, :]
        column = jnp.broadcast_to(row, (128, 256)).T
        item = iota((256, 128), 1).astype(F32)
        pick = jnp.concatenate([one(column == item + 128.0 * v) for v in range(8)], axis=1)
        rows = jnp.concatenate([dot(pick, wide(cat_ref, n)) for n in range(4)], axis=1)
        if half == 1:
            hid[...] = rows
        scale = lax.rsqrt(jnp.mean(rows * rows, axis=-1, keepdims=True) + EPS)
        normed = (rows * scale * gains_ref[0:1, :]).astype(BF).astype(F32)
        if half == 1:
            nf[16:272, :] = normed
        else:
            nf[0:16, :] = normed[240:256, :]
        nt[:, 256 * half:256 * half + 256] = normed.T


def windows(nt, first, u):
    def one_group(g, _):
        x = nt[pl.ds(16 * g, 16), :]
        for r in range(8):
            y = x if r == 0 else pltpu.roll(x, 512 - 16 * r, 1)
            for i in (r, r + 8):
                at = 0 if i < 8 else 128
                u[g, i] = (y[:, at:at + 256] * first[i:i + 1, :]).astype(BF)
        return 0

    lax.fori_loop(0, 64, one_group, 0)


def far_taps(u, h, live, far):
    lane = iota((256, 256), 1) % 16
    row = iota((256, 256), 0) % 16
    gap = (lane - row + 16) % 16
    t, q = iota((256, 256), 0), iota((256, 256), 1)
    spread = jnp.where(t == 16 * (q % 16) + q // 16, jnp.concatenate([live[...], live[...]], axis=1), 0.0).astype(BF)
    settle = one(q == 16 * ((t // 16 - t % 16 + 16) % 16) + t % 16)
    bit = iota((16, 128), 1)

    def one_block(s, _):
        w = jnp.zeros((256, 256), F32)
        for g in range(16):
            r = dot(u[16 * s + g].reshape(256, 256), h[16 * s + g])
            w = jnp.where(gap == g, r, w)
        halves = []
        for side in range(2):
            x = [w[16 * i:16 * i + 16, 128 * side:128 * side + 128] for i in range(16)]
            for b in range(4):
                step = 1 << b
                z = []
                for i in range(16):
                    if i & step:
                        z.append(jnp.where((bit & step) != 0, x[i], pltpu.roll(x[i ^ step], 128 - step, 1)))
                    else:
                        z.append(jnp.where((bit & step) == 0, x[i], pltpu.roll(x[i ^ step], step, 1)))
                x = z
            halves.append(jnp.concatenate(x, axis=0).astype(BF))
        turned = jnp.concatenate(halves, axis=1)
        far[s] = dot(dot_nt(spread, turned).astype(BF), settle)
        return 0

    lax.fori_loop(0, 4, one_block, 0)


def near_taps(tl_ref, taps_ref, keep, nf, hid, far):
    for s in range(8):
        cols = slice(128 * s, 128 * s + 128)
        w = jnp.where(iota((16, 128), 0) < tl_ref[:, cols], taps_ref[0:16, cols].astype(F32), 0.0)
        side = slice(128 * (s % 2), 128 * (s % 2) + 128)

        def rows(b, _):
            at = pl.multiple_of(64 * b, 64)
            x = nf[pl.ds(at, 80), cols]
            total = hid[pl.ds(at, 64), cols] + far[s // 2, pl.ds(at, 64), side]
            for lag in range(16):
                total = total + x[16 - lag:80 - lag, :] * (keep[lag, pl.ds(at, 64), :] * w[lag:lag + 1, :])
            hid[pl.ds(at, 64), cols] = total
            return 0

        lax.fori_loop(0, 4, rows, 0)


def feed_forward(gains_ref, w_ref, hid, inner, act, out_ref):
    rows = hid[...]
    scale = lax.rsqrt(jnp.mean(rows * rows, axis=-1, keepdims=True) + EPS)
    inner[...] = (rows * scale * gains_ref[1:2, :]).astype(BF)
    for n in range(4):
        cols = slice(256 * n, 256 * n + 256)
        gate = dot(inner[...], wide(w_ref.at[:, 0], n))
        up = dot(inner[...], wide(w_ref.at[:, 1], n))
        act[:, cols] = (gate / (1.0 + jnp.exp(-gate)) * up).astype(BF)
    for n in range(4):
        cols = slice(256 * n, 256 * n + 256)
        out_ref[:, cols] = (hid[:, cols] + dot(act[...], wide(w_ref.at[:, 2], n))).astype(BF)


def kernel(len_ref, ids_ref, tl_ref, taps_ref, gains_ref, cat_ref, w_ref,
           out_ref, hr, ht, h, keep, first, live, hid, nf, nt, u, far, inner, act):
    base = jnp.int32(0)
    for n, size in SIZES:
        base = base * size + lax.axis_index(n)
    base = base * 256
    prepare_taps(tl_ref, taps_ref, hr, ht, h)
    user_tables(base, len_ref, keep, first, live)
    look_up(ids_ref, cat_ref, gains_ref, hid, nf, nt)
    windows(nt, first, u)
    far_taps(u, h, live, far)
    near_taps(tl_ref, taps_ref, keep, nf, hid, far)
    feed_forward(gains_ref, w_ref, hid, inner, act, out_ref)


SCRATCH = [
    pltpu.VMEM((1024, 256), BF),
    pltpu.VMEM((64, 16, 16, 256), BF),
    pltpu.VMEM((64, 256, 256), BF),
    pltpu.VMEM((16, 256, 128), F32),
    pltpu.VMEM((16, 256), F32),
    pltpu.VMEM((256, 128), F32),
    pltpu.VMEM((256, 1024), F32),
    pltpu.VMEM((272, 1024), F32),
    pltpu.VMEM((1024, 512), F32),
    pltpu.VMEM((64, 16, 16, 256), BF),
    pltpu.VMEM((4, 256, 256), F32),
    pltpu.VMEM((256, 1024), BF),
    pltpu.VMEM((256, 1024), BF),
]


def compute(lens, ids2, tl, taps, gains, cat, w):
    vm = pl.BlockSpec(memory_space=pltpu.VMEM)
    sm = pl.BlockSpec(memory_space=pltpu.SMEM)
    return pl.pallas_call(
        kernel,
        out_shape=jax.ShapeDtypeStruct((256, 1024), BF),
        in_specs=[sm] + [vm] * 6,
        out_specs=vm,
        scratch_shapes=SCRATCH,
        compiler_params=pltpu.CompilerParams(vmem_limit_bytes=60 * 2**20),
    )(lens, ids2, tl, taps, gains, cat, w)


def body(item_ids, user_lengths, catalogue, tap_lengths, conv_taps, norm_gains, gate_weight, up_weight, down_weight):
    ids, catb, wb = gather(item_ids.reshape(1, 256), catalogue, gate_weight[0], up_weight[0], down_weight[0])
    return compute(user_lengths, ids.reshape(2, 256), tap_lengths, conv_taps[0], norm_gains[0],
                   catb.reshape(8, 1024, 128), wb.reshape(8, 3, 1024, 128))


def solution(mesh):
    finer = Mesh(mesh.devices.reshape([size for _, size in SIZES]), [name for name, _ in SIZES])
    every, col = ("x", "yl", "c", "z", "yh"), ("z", "yh")
    placed = (P(every), P(), P(every, None), P(), P(), P(), P(None, col, None), P(None, col, None), P(None, col, None))
    return jax.shard_map(body, mesh=finer, in_specs=placed, out_specs=P(every, None), check_vma=False)
```

```python
import jax
import jax.numpy as jnp
from jax import lax
from jax.experimental import pallas as pl
from jax.experimental.pallas import tpu as pltpu
from jax.sharding import Mesh
from jax.sharding import PartitionSpec as P

BF = jnp.bfloat16
F32 = jnp.float32
EPS = 1e-6
MESH = pl.DeviceIdType.MESH
NT = (((1,), (1,)), ((), ()))
SIZES = (("x", 4), ("yl", 2), ("c", 2), ("z", 8), ("yh", 4))
N_SEM = 224


class Net:
    def __init__(self, send, recv):
        self.send_sem, self.recv_sem, self.used, self.open = send, recv, 0, []
        self.at = {n: lax.axis_index(n) for n, _ in SIZES}

    def peer(self, **other):
        return {n: other.get(n, self.at[n]) for n, _ in SIZES}

    def step(self, distance):
        flat = jnp.int32(0)
        for n, size in SIZES:
            flat = flat * size + self.at[n]
        flat = lax.rem(flat + distance + 512, 512)
        out = {}
        for n, size in reversed(SIZES):
            out[n] = lax.rem(flat, size)
            flat = flat // size
        return out

    def copy(self, src, dst, to):
        k = self.used
        self.used += 1
        one = pltpu.make_async_remote_copy(
            src_ref=src, dst_ref=dst, send_sem=self.send_sem.at[k], recv_sem=self.recv_sem.at[k],
            device_id=to, device_id_type=MESH)
        one.start()
        self.open.append(one)
        return one

    def finish(self):
        for one in self.open:
            one.wait_send()


def geometry(net):
    a = net.at
    d = 2 * a["yl"] - 1
    e = 2 * lax.rem(a["z"], 2) - 1
    g = {}
    g["d"], g["e"] = d, e
    g["y_far"] = net.peer(yh=lax.rem(a["yh"] + d + 4, 4), yl=1 - a["yl"])
    g["y_near"] = net.peer(yl=1 - a["yl"])
    g["z_far"] = net.peer(z=lax.rem(a["z"] + e + 8, 8))
    g["z_near"] = net.peer(z=lax.rem(a["z"] - e + 8, 8))
    g["z_up"] = net.peer(z=lax.rem(a["z"] + 1, 8))
    g["z_down"] = net.peer(z=lax.rem(a["z"] + 7, 8))
    y = 2 * a["yh"] + a["yl"]
    up, down = lax.rem(y + 1, 8), lax.rem(y + 7, 8)
    g["y"] = y
    g["y_up"] = net.peer(yh=up // 2, yl=lax.rem(up, 2))
    g["y_down"] = net.peer(yh=down // 2, yl=lax.rem(down, 2))
    g["twin"] = net.peer(c=1 - a["c"])
    g["xs"] = [net.peer(x=lax.rem(a["x"] + s, 4)) for s in (1, 3, 2)]
    zh = a["z"] // 2
    g["zh"] = zh
    g["group"] = []
    for dc in range(2):
        for dz in range(2):
            for dy in range(4):
                if dc or dz or dy:
                    g["group"].append(net.peer(
                        c=lax.rem(a["c"] + dc, 2), z=2 * zh + lax.rem(a["z"] + dz, 2), yh=lax.rem(a["yh"] + dy, 4)))
    g["next"], g["prev"] = net.step(1), net.step(-1)
    return g


def entry_signals(g):
    barrier = pltpu.get_barrier_semaphore()
    near = g["group"] + g["xs"] + [g["y_far"], g["y_near"], g["z_far"], g["z_near"], g["y_up"], g["y_down"], g["z_up"], g["z_down"], g["next"], g["prev"]]
    for to in near:
        pl.semaphore_signal(barrier, inc=1, device_id=to, device_id_type=MESH)
    return len(near)


def pair_ring(block, h, d, count, far, near, net):
    one = net.copy(block(h), block(h), far)
    yield
    one.wait_recv()
    key = lax.rem(h + d + count, count)
    net.share_cat(block(key))
    one = net.copy(block(key), block(key), near)
    yield
    one.wait_recv()
    key = lax.rem(h - d + count, count)
    net.share_cat(block(key))
    one = net.copy(block(key), block(key), far)
    yield
    one.wait_recv()
    net.share_cat(block(lax.rem(h + 2, count)))


def ring_of_8(block, z, c, up, down, net):
    a = net.copy(block(z), block(z), up)
    b = net.copy(block(z), block(z), down)
    yield
    for hop in (1, 2):
        a.wait_recv()
        key = lax.rem(z - hop + 8, 8)
        net.share(block(key))
        a = net.copy(block(key), block(key), up)
        b.wait_recv()
        key = lax.rem(z + hop, 8)
        net.share(block(key))
        b = net.copy(block(key), block(key), down)
        yield
    a.wait_recv()
    net.share(block(lax.rem(z - 3 + 8, 8)))
    b.wait_recv()
    net.share(block(lax.rem(z + 3, 8)))
    key = lax.rem(z - 3 + 6 * c + 8, 8)
    to = {n: jnp.where(c == 0, up[n], down[n]) for n in up}
    a = net.copy(block(key), block(key), to)
    yield
    a.wait_recv()
    net.share(block(lax.rem(z + 4, 8)))


def dot(a, b):
    return jnp.dot(a, b, preferred_element_type=F32)


def dot_nt(a, b):
    return lax.dot_general(a, b, NT, preferred_element_type=F32)


def iota(shape, dim):
    return lax.broadcasted_iota(jnp.int32, shape, dim)


def one(cond):
    return jnp.where(cond, 1.0, 0.0).astype(BF)


def tap_rows(tl, taps, hr):
    p, k = iota((256, 256), 0), iota((256, 256), 1)
    reverse = one(p + k == 256)
    turned = one(k == 16 * (p // 16) + (p % 16 - p // 16 + 16) % 16)
    for s in range(4):
        cols = slice(256 * s, 256 * s + 256)
        table = jnp.where(p < tl[:, cols], taps[:, cols].astype(F32), 0.0).astype(BF)
        hr[cols, :] = dot_nt(turned, dot(reverse, table).astype(BF)).astype(BF)


def tap_shifts(hr, ht, begin, count):
    p, k = iota((256, 256), 0), iota((256, 256), 1)

    def shift_one(j, _):
        shift = one((k == p + j) & (p >= 1))
        for s in range(4):
            rows = dot(hr[256 * s:256 * s + 256, :], shift).astype(BF)
            ht[pl.ds(16 * s, 16), pl.ds(j, 1)] = rows.reshape(16, 1, 16, 256)
        return 0

    lax.fori_loop(begin, begin + count, shift_one, 0)


def tap_flips(ht, h, begin, count):
    unit = one(iota((256, 256), 0) == iota((256, 256), 1))

    def flip(g, _):
        for a in range(4):
            h[4 * g + a] = dot_nt(unit, ht[4 * g + a].reshape(256, 256)).astype(BF)
        return 0

    lax.fori_loop(begin, begin + count, flip, 0)


def user_tables(base, len_ref, keep, first, live):
    pos = base + iota((256, 128), 0)
    begin = jnp.zeros((256, 128), jnp.int32)
    pos_b = base + 16 * iota((16, 256), 0)
    begin_b = jnp.zeros((16, 256), jnp.int32)
    start = jnp.int32(0)
    for u in range(len_ref.shape[0]):
        begin = jnp.where(pos >= start, start, begin)
        begin_b = jnp.where(pos_b >= start, start, begin_b)
        start = start + len_ref[u]
    reach = jnp.minimum(pos - begin, iota((256, 128), 0) % 16)
    for lag in range(16):
        keep[lag] = jnp.where(lag <= reach, 1.0, 0.0)
    source = pos_b - 256 + iota((16, 256), 1)
    first[...] = jnp.where(source >= begin_b, 1.0, 0.0)
    head = base + 16 * (iota((256, 128), 0) // 16)
    live[...] = jnp.where(begin < head, 1.0, 0.0)


def wide(ref, n):
    return jnp.concatenate([ref[2 * n + k].reshape(1024, 128) for k in range(2)], axis=1)


def look_up(ids_ref, cat_ref, gains_ref, hid, nf, nt):
    ids = ids_ref[...].reshape(2, 256).astype(F32)
    for half in range(2):
        row = ids[half:half + 1, :]
        column = jnp.broadcast_to(row, (128, 256)).T
        item = iota((256, 128), 1).astype(F32)
        pick = jnp.concatenate([one(column == item + 128.0 * v) for v in range(8)], axis=1)
        rows = jnp.concatenate([dot(pick, wide(cat_ref, n)) for n in range(4)], axis=1)
        if half == 1:
            hid[...] = rows
        scale = lax.rsqrt(jnp.mean(rows * rows, axis=-1, keepdims=True) + EPS)
        normed = (rows * scale * gains_ref[0:1, :]).astype(BF).astype(F32)
        if half == 1:
            nf[16:272, :] = normed
        else:
            nf[0:16, :] = normed[240:256, :]
        nt[:, 256 * half:256 * half + 256] = normed.T


def windows(nt, first, u, begin, count):
    def one_group(n, _):
        for a in range(4):
            group(4 * n + a)
        return 0

    def group(g):
        x = nt[pl.ds(16 * g, 16), :]
        for r in range(8):
            y = x if r == 0 else pltpu.roll(x, 512 - 16 * r, 1)
            for i in (r, r + 8):
                at = 0 if i < 8 else 128
                u[g, i] = (y[:, at:at + 256] * first[i:i + 1, :]).astype(BF)

    lax.fori_loop(begin // 4, (begin + count) // 4, one_group, 0)


def far_taps(u, h, live, far, s):
    lane = iota((256, 256), 1) % 16
    row = iota((256, 256), 0) % 16
    gap = (lane - row + 16) % 16
    t, q = iota((256, 256), 0), iota((256, 256), 1)
    spread = jnp.where(t == 16 * (q % 16) + q // 16, jnp.concatenate([live[...], live[...]], axis=1), 0.0).astype(BF)
    settle = one(q == 16 * ((t // 16 - t % 16 + 16) % 16) + t % 16)
    bit = iota((16, 128), 1)

    def one_block():
        w = jnp.zeros((256, 256), F32)
        for g in range(16):
            r = dot(u[16 * s + g].reshape(256, 256), h[16 * s + g])
            w = jnp.where(gap == g, r, w)
        halves = []
        for side in range(2):
            x = [w[16 * i:16 * i + 16, 128 * side:128 * side + 128] for i in range(16)]
            for b in range(4):
                step = 1 << b
                z = []
                for i in range(16):
                    if i & step:
                        z.append(jnp.where((bit & step) != 0, x[i], pltpu.roll(x[i ^ step], 128 - step, 1)))
                    else:
                        z.append(jnp.where((bit & step) == 0, x[i], pltpu.roll(x[i ^ step], step, 1)))
                x = z
            halves.append(jnp.concatenate(x, axis=0).astype(BF))
        turned = jnp.concatenate(halves, axis=1)
        far[s] = dot(dot_nt(spread, turned).astype(BF), settle)

    one_block()


def near_taps(tl_ref, taps_ref, keep, nf, hid, far, parts):
    for s in parts:
        cols = slice(128 * s, 128 * s + 128)
        w = jnp.where(iota((16, 128), 0) < tl_ref[:, cols], taps_ref[0:16, cols].astype(F32), 0.0)
        side = slice(128 * (s % 2), 128 * (s % 2) + 128)

        def rows(b, _):
            at = pl.multiple_of(64 * b, 64)
            x = nf[pl.ds(at, 80), cols]
            total = hid[pl.ds(at, 64), cols] + far[s // 2, pl.ds(at, 64), side]
            for lag in range(16):
                total = total + x[16 - lag:80 - lag, :] * (keep[lag, pl.ds(at, 64), :] * w[lag:lag + 1, :])
            hid[pl.ds(at, 64), cols] = total
            return 0

        lax.fori_loop(0, 4, rows, 0)


def wide_w(ref, a, n):
    return jnp.concatenate([ref[2 * n + k, a].reshape(1024, 128) for k in range(2)], axis=1)


def feed_forward(gains_ref, w_ref, hid, inner, act, out_ref):
    rows = hid[...]
    scale = lax.rsqrt(jnp.mean(rows * rows, axis=-1, keepdims=True) + EPS)
    inner[...] = (rows * scale * gains_ref[1:2, :]).astype(BF)
    for n in range(4):
        cols = slice(256 * n, 256 * n + 256)
        gate = dot(inner[...], wide_w(w_ref, 0, n))
        up = dot(inner[...], wide_w(w_ref, 1, n))
        act[:, cols] = (gate / (1.0 + jnp.exp(-gate)) * up).astype(BF)
    for n in range(4):
        cols = slice(256 * n, 256 * n + 256)
        out_ref[:, cols] = (hid[:, cols] + dot(act[...], wide_w(w_ref, 2, n))).astype(BF)


def flows_of(net, g, catb, wb):
    a = net.at
    x, yl, c, z, yh, zh, y = a["x"], a["yl"], a["c"], a["z"], a["yh"], g["zh"], g["y"]
    lanes = pl.ds(4 * c, 4)

    def w_y_first(t):
        lt = 4 * c + t
        yield from ring_of_8(lambda k: wb.at[lt, :, z, k], y, c, g["y_up"], g["y_down"], net)
        yield from ring_of_8(lambda k: wb.at[lt, :, k], z, c, g["z_up"], g["z_down"], net)

    def w_z_first(t):
        lt = 4 * c + t
        yield from ring_of_8(lambda k: wb.at[lt, :, k, y], z, c, g["z_up"], g["z_down"], net)
        yield from ring_of_8(lambda k: wb.at[lt, :, :, k], y, c, g["y_up"], g["y_down"], net)

    def cat_x():
        net.share_cat(catb.at[lanes, x, yl, :, zh])
        ref = catb.at[lanes, x, yl, :, zh]
        out = [net.copy(ref, ref, to) for to in g["xs"]]
        yield
        for one_copy, s in zip(out, (1, 3, 2)):
            one_copy.wait_recv()
            net.share_cat(catb.at[lanes, lax.rem(x - s + 4, 4), yl, :, zh])

    def swap_y(part):
        first = net.copy(part(pl.ds(0, 2), yl), part(pl.ds(0, 2), yl), g["y_far"])
        second = net.copy(part(pl.ds(2, 2), yl), part(pl.ds(2, 2), yl), g["y_near"])
        yield
        first.wait_recv()
        second.wait_recv()
        net.share_cat(part(pl.ds(0, 4), 1 - yl))

    def cat_y_first():
        la = pl.ds(4 * c, 2)
        yield from swap_y(lambda xs, k: catb.at[la, xs, k, :, zh])
        yield from pair_ring(lambda h: catb.at[la, :, :, :, h], zh, g["e"], 4, g["z_far"], g["z_near"], net)

    def cat_z_first():
        la = pl.ds(4 * c + 2, 2)
        yield from pair_ring(lambda h: catb.at[la, :, yl, :, h], zh, g["e"], 4, g["z_far"], g["z_near"], net)
        yield from swap_y(lambda xs, k: catb.at[la, xs, k])

    return cat_x(), [cat_y_first(), cat_z_first()], [w_y_first(0), w_z_first(2), w_y_first(1), w_z_first(3)]


def tick(flows):
    for f in list(flows):
        try:
            next(f)
        except StopIteration:
            flows.remove(f)


def layer(len_hbm, ids_hbm, tl_hbm, taps_hbm, gains_hbm, cat_hbm, gate_hbm, up_hbm, down_hbm, out_ref,
          lens, ids, tl, taps, gains, pair, pairs, catb, wb, hr, ht, h, keep, first, live, hid, nf, nt, far, inner, act,
          load_sem, fill_sem, send, recv):
    net = Net(send, recv)
    g = geometry(net)
    a = net.at
    x, yl, c, z, yh, zh, y = a["x"], a["yl"], a["c"], a["z"], a["yh"], g["zh"], g["y"]
    loads = []
    for n, (src, dst) in enumerate(((cat_hbm, pair), (ids_hbm, ids.at[1]), (len_hbm, lens), (tl_hbm, tl), (gains_hbm, gains), (taps_hbm, taps))):
        loads.append(pltpu.make_async_copy(src, dst, load_sem.at[n]))
        loads[-1].start()
    fill = []
    mine = pl.ds(pl.multiple_of(16 * yl, 16), 16)
    for n, ref in enumerate((gate_hbm, up_hbm, down_hbm)):
        for t in range(8):
            fill.append(pltpu.make_async_copy(ref.at[mine, 128 * t:128 * t + 128], wb.at[t, n, z, y], fill_sem.at[8 * n + t]))
            fill[-1].start()
    near = entry_signals(g)
    loads[2].wait()
    base = jnp.int32(0)
    for n, size in SIZES:
        base = base * size + a[n]
    base = base * 256
    for k in (0, 1, 3, 4, 5):
        loads[k].wait()
    for one_copy in fill:
        one_copy.wait()
    pl.semaphore_wait(pltpu.get_barrier_semaphore(), near)

    shared, shared_cat = [], []
    net.share = lambda ref: shared.append(net.copy(ref, ref, g["twin"]))
    net.share_cat = lambda ref: shared_cat.append(net.copy(ref, ref, g["twin"]))
    cat_x, cats, weights = flows_of(net, g, catb, wb)
    slot = 4 * lax.rem(z, 2) + yh
    group = []
    for to in g["group"]:
        half = pl.ds(pl.multiple_of(512 * to["c"], 512), 512)
        group.append(net.copy(pair.at[:, half], pairs.at[c, slot], to))
    before = net.copy(ids.at[1], ids.at[0], g["next"])
    pairs[c, slot] = jnp.where(c == 0, pair[:, 0:512], pair[:, 512:1024])
    tick(weights)
    user_tables(base, lens, keep, first, live)
    tap_rows(tl, taps, hr)
    tap_shifts(hr, ht, 0, 2)
    for one_copy in group:
        one_copy.wait_recv()
    for k in range(2):
        rows = jnp.concatenate([pairs[k, i].astype(F32) for i in range(8)], axis=0).astype(BF)
        for t in range(4):
            catb[4 * c + t, x, yl, k, zh] = rows[:, 128 * t:128 * t + 128]
    tick(weights)
    next(cat_x)
    tap_shifts(hr, ht, 2, 5)
    tick([cat_x])
    tick(cats)
    tick(weights)
    tap_shifts(hr, ht, 7, 5)
    tick(cats)
    tick(weights)
    tap_shifts(hr, ht, 12, 4)
    tick(cats)
    tap_flips(ht, h, 0, 8)
    tick(cats)
    tick(weights)
    tap_flips(ht, h, 8, 8)
    tick(cats)
    tick(weights)
    while cats:
        tick(cats)
    before.wait_recv()
    for one_copy in shared_cat:
        one_copy.wait_recv()
    look_up(ids, catb, gains, hid, nf, nt)
    for s in range(4):
        tick(weights)
        windows(nt, first, ht, 16 * s, 16)
        far_taps(ht, h, live, far, s)
    tick(weights)
    near_taps(tl, taps, keep, nf, hid, far, range(8))
    while weights:
        tick(weights)
    for one_copy in shared:
        one_copy.wait_recv()
    feed_forward(gains, wb, hid, inner, act, out_ref)
    net.finish()


def body(item_ids, user_lengths, catalogue, tap_lengths, conv_taps, norm_gains, gate_weight, up_weight, down_weight):
    anywhere = pl.BlockSpec(memory_space=pl.ANY)
    return pl.pallas_call(
        layer,
        out_shape=jax.ShapeDtypeStruct((256, 1024), BF),
        in_specs=[anywhere] * 9,
        out_specs=pl.BlockSpec(memory_space=pltpu.VMEM),
        scratch_shapes=[
            pltpu.SMEM((32,), jnp.int32),
            pltpu.VMEM((2, 1, 256), jnp.int32),
            pltpu.VMEM((1, 1024), jnp.int32),
            pltpu.VMEM((256, 1024), BF),
            pltpu.VMEM((2, 1024), F32),
            pltpu.VMEM((2, 1024), BF),
            pltpu.VMEM((2, 8, 2, 512), BF),
            pltpu.VMEM((8, 4, 2, 2, 4, 16, 128), BF),
            pltpu.VMEM((8, 3, 8, 8, 16, 128), BF),
            pltpu.VMEM((1024, 256), BF),
            pltpu.VMEM((64, 16, 16, 256), BF),
            pltpu.VMEM((64, 256, 256), BF),
            pltpu.VMEM((16, 256, 128), F32),
            pltpu.VMEM((16, 256), F32),
            pltpu.VMEM((256, 128), F32),
            pltpu.VMEM((256, 1024), F32),
            pltpu.VMEM((272, 1024), F32),
            pltpu.VMEM((1024, 512), F32),
            pltpu.VMEM((4, 256, 256), F32),
            pltpu.VMEM((256, 1024), BF),
            pltpu.VMEM((256, 1024), BF),
            pltpu.SemaphoreType.DMA((6,)),
            pltpu.SemaphoreType.DMA((24,)),
            pltpu.SemaphoreType.DMA((N_SEM,)),
            pltpu.SemaphoreType.DMA((N_SEM,)),
        ],
        compiler_params=pltpu.CompilerParams(
            collective_id=0, has_side_effects=True, vmem_limit_bytes=66_000_000),
    )(user_lengths, item_ids.reshape(1, 256), tap_lengths, conv_taps[0], norm_gains[0], catalogue,
      gate_weight[0], up_weight[0], down_weight[0])


def solution(mesh):
    finer = Mesh(mesh.devices.reshape([size for _, size in SIZES]), [name for name, _ in SIZES])
    every, col = ("x", "yl", "c", "z", "yh"), ("z", "yh")
    placed = (P(every), P(), P(every, None), P(), P(), P(), P(None, col, None), P(None, col, None), P(None, col, None))
    return jax.shard_map(body, mesh=finer, in_specs=placed, out_specs=P(every, None), check_vma=False)
```

```python
import jax
import jax.numpy as jnp
from jax import lax
from jax.experimental import pallas as pl
from jax.experimental.pallas import tpu as pltpu
from jax.sharding import Mesh
from jax.sharding import PartitionSpec as P

BF = jnp.bfloat16
F32 = jnp.float32
EPS = 1e-6
MESH = pl.DeviceIdType.MESH
NT = (((1,), (1,)), ((), ()))
ORDER = "skew"
NT_DTYPE = BF
FIRST_DTYPE = BF
SIZES = (("x", 4), ("yl", 2), ("c", 2), ("z", 8), ("yh", 4))
N_SEM = 224


class Net:
    def __init__(self, send, recv):
        self.send_sem, self.recv_sem, self.used, self.open = send, recv, 0, []
        self.at = {n: lax.axis_index(n) for n, _ in SIZES}

    def peer(self, **other):
        return {n: other.get(n, self.at[n]) for n, _ in SIZES}

    def step(self, distance):
        flat = jnp.int32(0)
        for n, size in SIZES:
            flat = flat * size + self.at[n]
        flat = lax.rem(flat + distance + 512, 512)
        out = {}
        for n, size in reversed(SIZES):
            out[n] = lax.rem(flat, size)
            flat = flat // size
        return out

    def copy(self, src, dst, to):
        k = self.used
        self.used += 1
        one = pltpu.make_async_remote_copy(
            src_ref=src, dst_ref=dst, send_sem=self.send_sem.at[k], recv_sem=self.recv_sem.at[k],
            device_id=to, device_id_type=MESH)
        one.start()
        self.open.append(one)
        return one

    def finish(self):
        for one in self.open:
            one.wait_send()


def geometry(net):
    a = net.at
    d = 2 * a["yl"] - 1
    e = 2 * lax.rem(a["z"], 2) - 1
    g = {}
    g["d"], g["e"] = d, e
    g["y_far"] = net.peer(yh=lax.rem(a["yh"] + d + 4, 4), yl=1 - a["yl"])
    g["y_near"] = net.peer(yl=1 - a["yl"])
    g["z_far"] = net.peer(z=lax.rem(a["z"] + e + 8, 8))
    g["z_near"] = net.peer(z=lax.rem(a["z"] - e + 8, 8))
    g["z_up"] = net.peer(z=lax.rem(a["z"] + 1, 8))
    g["z_down"] = net.peer(z=lax.rem(a["z"] + 7, 8))
    y = 2 * a["yh"] + a["yl"]
    up, down = lax.rem(y + 1, 8), lax.rem(y + 7, 8)
    g["y"] = y
    g["y_up"] = net.peer(yh=up // 2, yl=lax.rem(up, 2))
    g["y_down"] = net.peer(yh=down // 2, yl=lax.rem(down, 2))
    g["ys"], g["zs"] = [], []
    for s in range(1, 8):
        to = lax.rem(y + s, 8)
        g["ys"].append(net.peer(yh=to // 2, yl=lax.rem(to, 2)))
        g["zs"].append(net.peer(z=lax.rem(a["z"] + s, 8)))
    g["z_run"] = [net.peer(z=lax.rem(a["z"] + s * e + 8, 8)) for s in (1, 2, 3)]
    g["twin"] = net.peer(c=1 - a["c"])
    g["xs"] = [net.peer(x=lax.rem(a["x"] + s, 4)) for s in (1, 3, 2)]
    zh = a["z"] // 2
    g["zh"] = zh
    g["group"] = []
    for dc in range(2):
        for dz in range(2):
            for dy in range(4):
                if dc or dz or dy:
                    g["group"].append(net.peer(
                        c=lax.rem(a["c"] + dc, 2), z=2 * zh + lax.rem(a["z"] + dz, 2), yh=lax.rem(a["yh"] + dy, 4)))
    g["next"], g["prev"] = net.step(1), net.step(-1)
    return g


def entry_signals(g):
    barrier = pltpu.get_barrier_semaphore()
    near = g["group"] + g["xs"] + g["ys"] + g["zs"] + [g["next"], g["prev"]]
    for to in near:
        pl.semaphore_signal(barrier, inc=1, device_id=to, device_id_type=MESH)
    return len(near)


def pair_ring(block, h, d, count, far, near, net):
    one = net.copy(block(h), block(h), far)
    yield
    one.wait_recv()
    key = lax.rem(h + d + count, count)
    net.share_cat(block(key))
    one = net.copy(block(key), block(key), near)
    yield
    one.wait_recv()
    key = lax.rem(h - d + count, count)
    net.share_cat(block(key))
    one = net.copy(block(key), block(key), far)
    yield
    one.wait_recv()
    net.share_cat(block(lax.rem(h + 2, count)))


def ring_of_8(block, z, c, up, down, net):
    a = net.copy(block(z), block(z), up)
    b = net.copy(block(z), block(z), down)
    yield
    for hop in (1, 2):
        a.wait_recv()
        key = lax.rem(z - hop + 8, 8)
        net.share(block(key))
        a = net.copy(block(key), block(key), up)
        b.wait_recv()
        key = lax.rem(z + hop, 8)
        net.share(block(key))
        b = net.copy(block(key), block(key), down)
        yield
    a.wait_recv()
    net.share(block(lax.rem(z - 3 + 8, 8)))
    b.wait_recv()
    net.share(block(lax.rem(z + 3, 8)))
    key = lax.rem(z - 3 + 6 * c + 8, 8)
    to = {n: jnp.where(c == 0, up[n], down[n]) for n in up}
    a = net.copy(block(key), block(key), to)
    yield
    a.wait_recv()
    net.share(block(lax.rem(z + 4, 8)))


def dot(a, b):
    return jnp.dot(a, b, preferred_element_type=F32)


def dot_nt(a, b):
    return lax.dot_general(a, b, NT, preferred_element_type=F32)


def iota(shape, dim):
    return lax.broadcasted_iota(jnp.int32, shape, dim)


def one(cond):
    return jnp.where(cond, 1.0, 0.0).astype(BF)


def tap_rows(tl, taps, hr):
    p, k = iota((256, 256), 0), iota((256, 256), 1)
    reverse = one(p + k == 256)
    turned = one(k == 16 * (p // 16) + (p % 16 - p // 16 + 16) % 16)
    for s in range(4):
        cols = slice(256 * s, 256 * s + 256)
        table = jnp.where(p < tl[:, cols], taps[:, cols].astype(F32), 0.0).astype(BF)
        hr[cols, :] = dot_nt(turned, dot(reverse, table).astype(BF)).astype(BF)


def tap_shifts(hr, ht, begin, count):
    p, k = iota((256, 256), 0), iota((256, 256), 1)

    def shift_one(j, _):
        shift = one((k == p + j) & (p >= 1))
        for s in range(4):
            rows = dot(hr[256 * s:256 * s + 256, :], shift).astype(BF)
            ht[pl.ds(16 * s, 16), pl.ds(j, 1)] = rows.reshape(16, 1, 16, 256)
        return 0

    lax.fori_loop(begin, begin + count, shift_one, 0)


def tap_flips(ht, h, begin, count):
    unit = one(iota((256, 256), 0) == iota((256, 256), 1))

    def flip(g, _):
        for a in range(4):
            h[4 * g + a] = dot_nt(unit, ht[4 * g + a].reshape(256, 256)).astype(BF)
        return 0

    lax.fori_loop(begin, begin + count, flip, 0)


def user_tables(base, len_ref, keep, first, live):
    pos = base + iota((256, 128), 0)
    begin = jnp.zeros((256, 128), jnp.int32)
    pos_b = base + 16 * iota((16, 256), 0)
    begin_b = jnp.zeros((16, 256), jnp.int32)
    start = jnp.int32(0)
    for u in range(len_ref.shape[0]):
        begin = jnp.where(pos >= start, start, begin)
        begin_b = jnp.where(pos_b >= start, start, begin_b)
        start = start + len_ref[u]
    reach = jnp.minimum(pos - begin, iota((256, 128), 0) % 16)
    for lag in range(16):
        keep[lag] = jnp.where(lag <= reach, 1.0, 0.0)
    source = pos_b - 256 + iota((16, 256), 1)
    first[...] = jnp.where(source >= begin_b, 1.0, 0.0).astype(BF)
    head = base + 16 * (iota((256, 128), 0) // 16)
    live[...] = jnp.where(begin < head, 1.0, 0.0)


def wide(ref, n):
    return jnp.concatenate([ref[2 * n + k].reshape(1024, 128) for k in range(2)], axis=1)


def look_up(ids_ref, cat_ref, gains_ref, hid, nf, nt):
    ids = ids_ref[...].reshape(2, 256).astype(F32)
    for half in range(2):
        row = ids[half:half + 1, :]
        column = jnp.broadcast_to(row, (128, 256)).T
        item = iota((256, 128), 1).astype(F32)
        pick = jnp.concatenate([one(column == item + 128.0 * v) for v in range(8)], axis=1)
        rows = jnp.concatenate([dot(pick, wide(cat_ref, n)) for n in range(4)], axis=1)
        if half == 1:
            hid[...] = rows
        scale = lax.rsqrt(jnp.mean(rows * rows, axis=-1, keepdims=True) + EPS)
        normed = (rows * scale * gains_ref[0:1, :]).astype(BF).astype(F32)
        if half == 1:
            nf[16:272, :] = normed
        else:
            nf[0:16, :] = normed[240:256, :]
        nt[:, 256 * half:256 * half + 256] = normed.astype(BF).T


def windows(nt, first, u, begin, count):
    def one_group(n, _):
        for a in range(4):
            group(4 * n + a)
        return 0

    def group(g):
        x = nt[pl.ds(16 * g, 16), :]
        for r in range(8):
            y = x if r == 0 else pltpu.roll(x, 512 - 16 * r, 1)
            for i in (r, r + 8):
                at = 0 if i < 8 else 128
                u[g, i] = y[:, at:at + 256] * first[i:i + 1, :]

    for n in range(begin // 4, (begin + count) // 4):
        one_group(n, 0)


def far_taps(u, h, live, far, s):
    lane = iota((256, 256), 1) % 16
    row = iota((256, 256), 0) % 16
    gap = (lane - row + 16) % 16
    t, q = iota((256, 256), 0), iota((256, 256), 1)
    spread = jnp.where(t == 16 * (q % 16) + q // 16, jnp.concatenate([live[...], live[...]], axis=1), 0.0).astype(BF)
    settle = one(q == 16 * ((t // 16 - t % 16 + 16) % 16) + t % 16)
    bit = iota((16, 128), 1)

    def one_block():
        w = jnp.zeros((256, 256), F32)
        for g in range(16):
            r = dot(u[16 * s + g].reshape(256, 256), h[16 * s + g])
            w = jnp.where(gap == g, r, w)
        halves = []
        for side in range(2):
            x = [w[16 * i:16 * i + 16, 128 * side:128 * side + 128] for i in range(16)]
            for b in range(4):
                step = 1 << b
                z = []
                for i in range(16):
                    if i & step:
                        z.append(jnp.where((bit & step) != 0, x[i], pltpu.roll(x[i ^ step], 128 - step, 1)))
                    else:
                        z.append(jnp.where((bit & step) == 0, x[i], pltpu.roll(x[i ^ step], step, 1)))
                x = z
            halves.append(jnp.concatenate(x, axis=0).astype(BF))
        turned = jnp.concatenate(halves, axis=1)
        far[s] = dot(dot_nt(spread, turned).astype(BF), settle)

    one_block()


def near_taps(tl_ref, taps_ref, keep, nf, hid, parts):
    for s in parts:
        cols = slice(128 * s, 128 * s + 128)
        w = jnp.where(iota((16, 128), 0) < tl_ref[:, cols], taps_ref[0:16, cols].astype(F32), 0.0)
        for b in range(4):
            rows = slice(64 * b, 64 * b + 64)
            x = nf[64 * b:64 * b + 80, cols]
            total = hid[rows, cols]
            for lag in range(16):
                total = total + x[16 - lag:80 - lag, :] * (keep[lag, rows, :] * w[lag:lag + 1, :])
            hid[rows, cols] = total


def wide_w(ref, a, n):
    return jnp.concatenate([ref[2 * n + k, a].reshape(1024, 128) for k in range(2)], axis=1)


def feed_forward(gains_ref, w_ref, far, hid, inner, act, out_ref):
    rows = hid[...] + jnp.concatenate([far[s] for s in range(4)], axis=1)
    hid[...] = rows
    scale = lax.rsqrt(jnp.mean(rows * rows, axis=-1, keepdims=True) + EPS)
    inner[...] = (rows * scale * gains_ref[1:2, :]).astype(BF)
    for n in range(4):
        cols = slice(256 * n, 256 * n + 256)
        gate = dot(inner[...], wide_w(w_ref, 0, n))
        up = dot(inner[...], wide_w(w_ref, 1, n))
        act[:, cols] = (gate / (1.0 + jnp.exp(-gate)) * up).astype(BF)
    for n in range(4):
        cols = slice(256 * n, 256 * n + 256)
        out_ref[:, cols] = (hid[:, cols] + dot(act[...], wide_w(w_ref, 2, n))).astype(BF)


def pair_run(block, h, e, targets, net):
    out = [net.copy(block(h), block(h), to) for to in targets]
    yield
    yield
    for one_copy, key in zip(out, (h + e + 4, h - e + 4, h + 2)):
        one_copy.wait_recv()
        net.share_cat(block(lax.rem(key, 4)))


def all_of_8(block, whole, k, targets, net):
    out = [net.copy(block(k), block(k), to) for to in targets]
    yield
    for one_copy in out:
        one_copy.wait_recv()
    net.share(whole)


def ring_of_4(block, x, c, up, down, share, net):
    a = net.copy(block(x), block(x), up)
    b = net.copy(block(x), block(x), down)
    yield
    a.wait_recv()
    b.wait_recv()
    key = lax.rem(x + 3 + 2 * c, 4)
    to = {n: jnp.where(c == 0, up[n], down[n]) for n in up}
    a = net.copy(block(key), block(key), to)
    share(block(lax.rem(x + 3, 4)))
    share(block(lax.rem(x + 1, 4)))
    yield
    a.wait_recv()
    share(block(lax.rem(x + 2, 4)))


def flows_of(net, g, catb, wb):
    a = net.at
    x, yl, c, z, yh, zh, y = a["x"], a["yl"], a["c"], a["z"], a["yh"], g["zh"], g["y"]
    t_a, t_b, t_c = 4 * c, 4 * c + 1, pl.ds(4 * c + 2, 2)

    def w_a():
        yield from all_of_8(lambda k: wb.at[t_a, :, z, k], wb.at[t_a, :, z], y, g["ys"], net)
        yield from ring_of_8(lambda k: wb.at[t_a, :, k], z, c, g["z_up"], g["z_down"], net)

    def w_b():
        yield from all_of_8(lambda k: wb.at[t_b, :, k, y], wb.at[t_b, :, :, y], z, g["zs"], net)
        yield from ring_of_8(lambda k: wb.at[t_b, :, :, k], y, c, g["y_up"], g["y_down"], net)

    def quarter(of, zs, ys):
        rows = pl.ds(pl.multiple_of(8 * (of // 2), 8), 8)
        return wb.at[4 * c + 2 + lax.rem(of, 2), :, zs, ys, rows]

    def w_c():
        every = pl.ds(0, 8)
        yield from all_of_8(lambda k: quarter(x, z, k), quarter(x, z, every), y, g["ys"], net)
        ring = ring_of_8(lambda k: quarter(x, k, every), z, c, g["z_up"], g["z_down"], net)
        across = []
        for keys in ((0,), (7, 1), (6, 2), (5, 3), (4,)):
            more = next(ring, 0) is None
            for f in list(across):
                if next(f, 0) == 0:
                    across.remove(f)
            for k in keys:
                key = lax.rem(z + k, 8)
                f = ring_of_4(lambda of, key=key: quarter(of, key, every), x, c, g["xs"][0], g["xs"][1], net.share, net)
                next(f)
                across.append(f)
            yield
        while across:
            for f in list(across):
                if next(f, 0) == 0:
                    across.remove(f)
            yield

    def swap_y(first, second, both):
        one_copy = net.copy(first, first, g["y_far"])
        two = net.copy(second, second, g["y_near"])
        yield
        one_copy.wait_recv()
        two.wait_recv()
        net.share_cat(both)

    def cat_ab():
        net.share_cat(catb.at[pl.ds(4 * c, 4), x, yl, :, zh])
        ref = catb.at[pl.ds(4 * c, 2), x, yl, :, zh]
        out = [net.copy(ref, ref, to) for to in g["xs"]]
        yield
        for one_copy, s in zip(out, (1, 3, 2)):
            one_copy.wait_recv()
            net.share_cat(catb.at[pl.ds(4 * c, 2), lax.rem(x - s + 4, 4), yl, :, zh])
        both = [cat_a(), cat_b()]
        while both:
            tick(both)
            yield

    def cat_a():
        yield from swap_y(catb.at[t_a, pl.ds(0, 2), yl, :, zh], catb.at[t_a, pl.ds(2, 2), yl, :, zh],
                          catb.at[t_a, :, 1 - yl, :, zh])
        yield from pair_ring(lambda h: catb.at[t_a, :, :, :, h], zh, g["e"], 4, g["z_far"], g["z_near"], net)

    def cat_b():
        yield from pair_run(lambda h: catb.at[t_b, :, yl, :, h], zh, g["e"], g["z_run"], net)
        yield from swap_y(catb.at[t_b, pl.ds(0, 2), yl], catb.at[t_b, pl.ds(2, 2), yl], catb.at[t_b, :, 1 - yl])

    def cat_c():
        yield from pair_run(lambda h: catb.at[t_c, x, yl, :, h], zh, g["e"], g["z_run"], net)
        yield from swap_y(catb.at[t_c, x, yl, 0], catb.at[t_c, x, yl, 1], catb.at[t_c, x, 1 - yl])
        yield from ring_of_4(lambda k: catb.at[t_c, k], x, c, g["xs"][0], g["xs"][1], net.share_cat, net)

    return [cat_c(), cat_ab()], [w_a(), w_b(), w_c()]


def tick(flows):
    for f in list(flows):
        try:
            next(f)
        except StopIteration:
            flows.remove(f)


def layer(len_hbm, ids_hbm, tl_hbm, taps_hbm, gains_hbm, cat_hbm, gate_hbm, up_hbm, down_hbm, out_ref,
          lens, ids, tl, taps, gains, pair, pairs, catb, wb, hr, ht, h, keep, first, live, hid, nf, nt, far, inner, act,
          load_sem, fill_sem, send, recv):
    net = Net(send, recv)
    g = geometry(net)
    a = net.at
    x, yl, c, z, yh, zh, y = a["x"], a["yl"], a["c"], a["z"], a["yh"], g["zh"], g["y"]
    loads = []
    for n, (src, dst) in enumerate(((cat_hbm, pair), (ids_hbm, ids.at[1]), (len_hbm, lens), (tl_hbm, tl), (gains_hbm, gains), (taps_hbm, taps))):
        loads.append(pltpu.make_async_copy(src, dst, load_sem.at[n]))
        loads[-1].start()
    fill = []
    mine = pl.ds(pl.multiple_of(16 * yl, 16), 16)
    part = pl.ds(pl.multiple_of(8 * (x // 2), 8), 8)
    mine_part = pl.ds(pl.multiple_of(16 * yl + 8 * (x // 2), 8), 8)
    third = 2 + lax.rem(x, 2)
    for n, ref in enumerate((gate_hbm, up_hbm, down_hbm)):
        for t in range(3):
            if t < 2:
                src = ref.at[mine, pl.ds(pl.multiple_of(512 * c + 128 * t, 128), 128)]
                dst = wb.at[4 * c + t, n, z, y]
            else:
                src = ref.at[mine_part, pl.ds(pl.multiple_of(512 * c + 128 * third, 128), 128)]
                dst = wb.at[4 * c + third, n, z, y, part]
            fill.append(pltpu.make_async_copy(src, dst, fill_sem.at[3 * n + t]))
            fill[-1].start()
    near = entry_signals(g)
    loads[2].wait()
    base = jnp.int32(0)
    for n, size in SIZES:
        base = base * size + a[n]
    base = base * 256
    for k in (0, 1, 3, 4, 5):
        loads[k].wait()
    for one_copy in fill:
        one_copy.wait()
    pl.semaphore_wait(pltpu.get_barrier_semaphore(), near)

    shared, shared_cat = [], []
    net.share = lambda ref: shared.append(net.copy(ref, ref, g["twin"]))
    net.share_cat = lambda ref: shared_cat.append(net.copy(ref, ref, g["twin"]))
    cats, weights = flows_of(net, g, catb, wb)
    slot = 4 * lax.rem(z, 2) + yh
    group = []
    for to in g["group"]:
        half = pl.ds(pl.multiple_of(512 * to["c"], 512), 512)
        group.append(net.copy(pair.at[:, half], pairs.at[c, slot], to))
    before = net.copy(ids.at[1], ids.at[0], g["next"])
    pairs[c, slot] = jnp.where(c == 0, pair[:, 0:512], pair[:, 512:1024])
    tick(weights)
    user_tables(base, lens, keep, first, live)
    tap_rows(tl, taps, hr)
    tap_shifts(hr, ht, 0, 3)
    for one_copy in group:
        one_copy.wait_recv()
    for k in range(2):
        rows = jnp.concatenate([pairs[k, i].astype(F32) for i in range(8)], axis=0).astype(BF)
        for t in range(4):
            catb[4 * c + t, x, yl, k, zh] = rows[:, 128 * t:128 * t + 128]
    tick(cats)
    tick(weights)
    tap_shifts(hr, ht, 3, 5)
    tick(cats)
    tap_shifts(hr, ht, 8, 5)
    tick(cats)
    tick(weights)
    tap_shifts(hr, ht, 13, 3)
    tap_flips(ht, h, 0, 4)
    tick(cats)
    tick(weights)
    tap_flips(ht, h, 4, 6)
    tick(cats)
    tick(weights)
    tap_flips(ht, h, 10, 6)
    while cats:
        tick(cats)
    before.wait_recv()
    for one_copy in shared_cat:
        one_copy.wait_recv()
    look_up(ids, catb, gains, hid, nf, nt)
    tick(weights)
    windows(nt, first, ht, 0, 16)
    for s in range(4):
        tick(weights)
        if s < 3:
            windows(nt, first, ht, 16 * s + 16, 16)
        near_taps(tl, taps, keep, nf, hid, (2 * s, 2 * s + 1))
        far_taps(ht, h, live, far, s)
    while weights:
        tick(weights)
    for one_copy in shared:
        one_copy.wait_recv()
    feed_forward(gains, wb, far, hid, inner, act, out_ref)
    net.finish()


def body(item_ids, user_lengths, catalogue, tap_lengths, conv_taps, norm_gains, gate_weight, up_weight, down_weight):
    anywhere = pl.BlockSpec(memory_space=pl.ANY)
    return pl.pallas_call(
        layer,
        out_shape=jax.ShapeDtypeStruct((256, 1024), BF),
        in_specs=[anywhere] * 9,
        out_specs=pl.BlockSpec(memory_space=pltpu.VMEM),
        scratch_shapes=[
            pltpu.SMEM((32,), jnp.int32),
            pltpu.VMEM((2, 1, 256), jnp.int32),
            pltpu.VMEM((1, 1024), jnp.int32),
            pltpu.VMEM((256, 1024), BF),
            pltpu.VMEM((2, 1024), F32),
            pltpu.VMEM((2, 1024), BF),
            pltpu.VMEM((2, 8, 2, 512), BF),
            pltpu.VMEM((8, 4, 2, 2, 4, 16, 128), BF),
            pltpu.VMEM((8, 3, 8, 8, 16, 128), BF),
            pltpu.VMEM((1024, 256), BF),
            pltpu.VMEM((64, 16, 16, 256), BF),
            pltpu.VMEM((64, 256, 256), BF),
            pltpu.VMEM((16, 256, 128), F32),
            pltpu.VMEM((16, 256), BF),
            pltpu.VMEM((256, 128), F32),
            pltpu.VMEM((256, 1024), F32),
            pltpu.VMEM((272, 1024), F32),
            pltpu.VMEM((1024, 512), BF),
            pltpu.VMEM((4, 256, 256), F32),
            pltpu.VMEM((256, 1024), BF),
            pltpu.VMEM((256, 1024), BF),
            pltpu.SemaphoreType.DMA((6,)),
            pltpu.SemaphoreType.DMA((9,)),
            pltpu.SemaphoreType.DMA((N_SEM,)),
            pltpu.SemaphoreType.DMA((N_SEM,)),
        ],
        compiler_params=pltpu.CompilerParams(
            collective_id=0, has_side_effects=True, vmem_limit_bytes=66_000_000),
    )(user_lengths, item_ids.reshape(1, 256), tap_lengths, conv_taps[0], norm_gains[0], catalogue,
      gate_weight[0], up_weight[0], down_weight[0])


def solution(mesh):
    finer = Mesh(mesh.devices.reshape([size for _, size in SIZES]), [name for name, _ in SIZES])
    every, col = ("x", "yl", "c", "z", "yh"), ("z", "yh")
    placed = (P(every), P(), P(every, None), P(), P(), P(), P(None, col, None), P(None, col, None), P(None, col, None))
    return jax.shard_map(body, mesh=finer, in_specs=placed, out_specs=P(every, None), check_vma=False)
```

```python
import jax
import jax.numpy as jnp
from jax import lax
from jax.experimental import pallas as pl
from jax.experimental.pallas import tpu as pltpu
from jax.sharding import Mesh
from jax.sharding import PartitionSpec as P

BF = jnp.bfloat16
F32 = jnp.float32
EPS = 1e-6
MESH = pl.DeviceIdType.MESH
NT = (((1,), (1,)), ((), ()))
ORDER = "skew"
NT_DTYPE = BF
FIRST_DTYPE = BF
SIZES = (("x", 4), ("yl", 2), ("c", 2), ("z", 8), ("yh", 4))
N_SEM = 224


class Net:
    def __init__(self, send, recv):
        self.send_sem, self.recv_sem, self.used, self.open = send, recv, 0, []
        self.at = {n: lax.axis_index(n) for n, _ in SIZES}

    def peer(self, **other):
        return {n: other.get(n, self.at[n]) for n, _ in SIZES}

    def step(self, distance):
        flat = jnp.int32(0)
        for n, size in SIZES:
            flat = flat * size + self.at[n]
        flat = lax.rem(flat + distance + 512, 512)
        out = {}
        for n, size in reversed(SIZES):
            out[n] = lax.rem(flat, size)
            flat = flat // size
        return out

    def copy(self, src, dst, to):
        k = self.used
        self.used += 1
        one = pltpu.make_async_remote_copy(
            src_ref=src, dst_ref=dst, send_sem=self.send_sem.at[k], recv_sem=self.recv_sem.at[k],
            device_id=to, device_id_type=MESH)
        one.start()
        self.open.append(one)
        return one

    def finish(self):
        for one in self.open:
            one.wait_send()


def geometry(net):
    a = net.at
    d = 2 * a["yl"] - 1
    e = 2 * lax.rem(a["z"], 2) - 1
    g = {}
    g["d"], g["e"] = d, e
    g["y_far"] = net.peer(yh=lax.rem(a["yh"] + d + 4, 4), yl=1 - a["yl"])
    g["y_near"] = net.peer(yl=1 - a["yl"])
    g["z_far"] = net.peer(z=lax.rem(a["z"] + e + 8, 8))
    g["z_near"] = net.peer(z=lax.rem(a["z"] - e + 8, 8))
    g["z_up"] = net.peer(z=lax.rem(a["z"] + 1, 8))
    g["z_down"] = net.peer(z=lax.rem(a["z"] + 7, 8))
    y = 2 * a["yh"] + a["yl"]
    up, down = lax.rem(y + 1, 8), lax.rem(y + 7, 8)
    g["y"] = y
    g["y_up"] = net.peer(yh=up // 2, yl=lax.rem(up, 2))
    g["y_down"] = net.peer(yh=down // 2, yl=lax.rem(down, 2))
    g["ys"], g["zs"] = [], []
    for s in range(1, 8):
        to = lax.rem(y + s, 8)
        g["ys"].append(net.peer(yh=to // 2, yl=lax.rem(to, 2)))
        g["zs"].append(net.peer(z=lax.rem(a["z"] + s, 8)))
    g["z_run"] = [net.peer(z=lax.rem(a["z"] + s * e + 8, 8)) for s in (1, 2, 3)]
    g["twin"] = net.peer(c=1 - a["c"])
    g["xs"] = [net.peer(x=lax.rem(a["x"] + s, 4)) for s in (1, 3, 2)]
    zh = a["z"] // 2
    g["zh"] = zh
    g["group"] = []
    for dc in range(2):
        for dz in range(2):
            for dy in range(4):
                if dc or dz or dy:
                    g["group"].append(net.peer(
                        c=lax.rem(a["c"] + dc, 2), z=2 * zh + lax.rem(a["z"] + dz, 2), yh=lax.rem(a["yh"] + dy, 4)))
    g["next"], g["prev"] = net.step(1), net.step(-1)
    return g


def entry_signals(g):
    barrier = pltpu.get_barrier_semaphore()
    near = g["group"] + g["xs"] + g["ys"] + g["zs"] + [g["next"], g["prev"]]
    for to in near:
        pl.semaphore_signal(barrier, inc=1, device_id=to, device_id_type=MESH)
    return len(near)


def pair_ring(block, h, d, count, far, near, net):
    one = net.copy(block(h), block(h), far)
    yield
    one.wait_recv()
    key = lax.rem(h + d + count, count)
    net.share_cat(block(key))
    one = net.copy(block(key), block(key), near)
    yield
    one.wait_recv()
    key = lax.rem(h - d + count, count)
    net.share_cat(block(key))
    one = net.copy(block(key), block(key), far)
    yield
    one.wait_recv()
    net.share_cat(block(lax.rem(h + 2, count)))


def ring_of_8(block, z, c, up, down, net):
    a = net.copy(block(z), block(z), up)
    b = net.copy(block(z), block(z), down)
    yield
    for hop in (1, 2):
        a.wait_recv()
        key = lax.rem(z - hop + 8, 8)
        net.share(block(key))
        a = net.copy(block(key), block(key), up)
        b.wait_recv()
        key = lax.rem(z + hop, 8)
        net.share(block(key))
        b = net.copy(block(key), block(key), down)
        yield
    a.wait_recv()
    net.share(block(lax.rem(z - 3 + 8, 8)))
    b.wait_recv()
    net.share(block(lax.rem(z + 3, 8)))
    key = lax.rem(z - 3 + 6 * c + 8, 8)
    to = {n: jnp.where(c == 0, up[n], down[n]) for n in up}
    a = net.copy(block(key), block(key), to)
    yield
    a.wait_recv()
    net.share(block(lax.rem(z + 4, 8)))


def dot(a, b):
    return jnp.dot(a, b, preferred_element_type=F32)


def dot_nt(a, b):
    return lax.dot_general(a, b, NT, preferred_element_type=F32)


def iota(shape, dim):
    return lax.broadcasted_iota(jnp.int32, shape, dim)


def one(cond):
    return jnp.where(cond, 1.0, 0.0).astype(BF)


def tap_rows(tl, taps, hr):
    p, k = iota((256, 256), 0), iota((256, 256), 1)
    reverse = one(p + k == 256)
    turned = one(k == 16 * (p // 16) + (p % 16 - p // 16 + 16) % 16)
    for s in range(4):
        cols = slice(256 * s, 256 * s + 256)
        table = jnp.where(p < tl[:, cols], taps[:, cols].astype(F32), 0.0).astype(BF)
        hr[cols, :] = dot_nt(turned, dot(reverse, table).astype(BF)).astype(BF)


def tap_shifts(hr, ht, begin, count):
    p, k = iota((256, 256), 0), iota((256, 256), 1)

    def shift_one(j, _):
        shift = one((k == p + j) & (p >= 1))
        for s in range(4):
            rows = dot(hr[256 * s:256 * s + 256, :], shift).astype(BF)
            ht[pl.ds(16 * s, 16), pl.ds(j, 1)] = rows.reshape(16, 1, 16, 256)
        return 0

    lax.fori_loop(begin, begin + count, shift_one, 0)


def tap_flips(ht, h, begin, count):
    unit = one(iota((256, 256), 0) == iota((256, 256), 1))

    def flip(g, _):
        for a in range(4):
            h[4 * g + a] = dot_nt(unit, ht[4 * g + a].reshape(256, 256)).astype(BF)
        return 0

    lax.fori_loop(begin, begin + count, flip, 0)


def user_tables(base, len_ref, keep, first, live):
    pos = base + iota((256, 128), 0)
    begin = jnp.zeros((256, 128), jnp.int32)
    pos_b = base + 16 * iota((16, 256), 0)
    begin_b = jnp.zeros((16, 256), jnp.int32)
    start = jnp.int32(0)
    for u in range(len_ref.shape[0]):
        begin = jnp.where(pos >= start, start, begin)
        begin_b = jnp.where(pos_b >= start, start, begin_b)
        start = start + len_ref[u]
    reach = jnp.minimum(pos - begin, iota((256, 128), 0) % 16)
    for lag in range(16):
        keep[lag] = jnp.where(lag <= reach, 1.0, 0.0)
    source = pos_b - 256 + iota((16, 256), 1)
    first[...] = jnp.where(source >= begin_b, 1.0, 0.0).astype(BF)
    head = base + 16 * (iota((256, 128), 0) // 16)
    live[...] = jnp.where(begin < head, 1.0, 0.0)


def wide(ref, n):
    return jnp.concatenate([ref[2 * n + k].reshape(1024, 128) for k in range(2)], axis=1)


def look_up(ids_ref, cat_ref, gains_ref, hid, nf, nt):
    ids = ids_ref[...].reshape(2, 256).astype(F32)
    for half in range(2):
        row = ids[half:half + 1, :]
        column = jnp.broadcast_to(row, (128, 256)).T
        item = iota((256, 128), 1).astype(F32)
        pick = jnp.concatenate([one(column == item + 128.0 * v) for v in range(8)], axis=1)
        rows = jnp.concatenate([dot(pick, wide(cat_ref, n)) for n in range(4)], axis=1)
        if half == 1:
            hid[...] = rows
        scale = lax.rsqrt(jnp.mean(rows * rows, axis=-1, keepdims=True) + EPS)
        normed = (rows * scale * gains_ref[0:1, :]).astype(BF).astype(F32)
        if half == 1:
            nf[16:272, :] = normed
        else:
            nf[0:16, :] = normed[240:256, :]
        nt[:, 256 * half:256 * half + 256] = normed.astype(BF).T


def windows(nt, first, u, begin, count):
    def one_group(n, _):
        for a in range(4):
            group(4 * n + a)
        return 0

    def group(g):
        x = nt[pl.ds(16 * g, 16), :]
        for r in range(8):
            y = x if r == 0 else pltpu.roll(x, 512 - 16 * r, 1)
            for i in (r, r + 8):
                at = 0 if i < 8 else 128
                u[g, i] = y[:, at:at + 256] * first[i:i + 1, :]

    for n in range(begin // 4, (begin + count) // 4):
        one_group(n, 0)


def far_taps(u, h, live, far, s):
    lane = iota((256, 256), 1) % 16
    row = iota((256, 256), 0) % 16
    gap = (lane - row + 16) % 16
    t, q = iota((256, 256), 0), iota((256, 256), 1)
    spread = jnp.where(t == 16 * (q % 16) + q // 16, jnp.concatenate([live[...], live[...]], axis=1), 0.0).astype(BF)
    settle = one(q == 16 * ((t // 16 - t % 16 + 16) % 16) + t % 16)
    bit = iota((16, 128), 1)

    def one_block():
        w = jnp.zeros((256, 256), F32)
        for g in range(16):
            r = dot(u[16 * s + g].reshape(256, 256), h[16 * s + g])
            w = jnp.where(gap == g, r, w)
        halves = []
        for side in range(2):
            x = [w[16 * i:16 * i + 16, 128 * side:128 * side + 128] for i in range(16)]
            for b in range(4):
                step = 1 << b
                z = []
                for i in range(16):
                    if i & step:
                        z.append(jnp.where((bit & step) != 0, x[i], pltpu.roll(x[i ^ step], 128 - step, 1)))
                    else:
                        z.append(jnp.where((bit & step) == 0, x[i], pltpu.roll(x[i ^ step], step, 1)))
                x = z
            halves.append(jnp.concatenate(x, axis=0).astype(BF))
        turned = jnp.concatenate(halves, axis=1)
        far[s] = dot(dot_nt(spread, turned).astype(BF), settle)

    one_block()


def near_taps(tl_ref, taps_ref, keep, nf, hid, parts):
    for s in parts:
        cols = slice(128 * s, 128 * s + 128)
        w = jnp.where(iota((16, 128), 0) < tl_ref[:, cols], taps_ref[0:16, cols].astype(F32), 0.0)
        for b in range(4):
            rows = slice(64 * b, 64 * b + 64)
            x = nf[64 * b:64 * b + 80, cols]
            total = hid[rows, cols]
            for lag in range(16):
                total = total + x[16 - lag:80 - lag, :] * (keep[lag, rows, :] * w[lag:lag + 1, :])
            hid[rows, cols] = total


def wide_w(ref, a, n):
    return jnp.concatenate([ref[2 * n + k, a].reshape(1024, 128) for k in range(2)], axis=1)


def feed_forward(gains_ref, w_ref, far, hid, inner, act, out_ref):
    rows = hid[...] + jnp.concatenate([far[s] for s in range(4)], axis=1)
    hid[...] = rows
    scale = lax.rsqrt(jnp.mean(rows * rows, axis=-1, keepdims=True) + EPS)
    inner[...] = (rows * scale * gains_ref[1:2, :]).astype(BF)
    for n in range(4):
        cols = slice(256 * n, 256 * n + 256)
        gate = dot(inner[...], wide_w(w_ref, 0, n))
        up = dot(inner[...], wide_w(w_ref, 1, n))
        act[:, cols] = (gate / (1.0 + jnp.exp(-gate)) * up).astype(BF)
    for n in range(4):
        cols = slice(256 * n, 256 * n + 256)
        out_ref[:, cols] = (hid[:, cols] + dot(act[...], wide_w(w_ref, 2, n))).astype(BF)


def pair_run(block, h, e, targets, net):
    out = [net.copy(block(h), block(h), to) for to in targets]
    yield
    yield
    for one_copy, key in zip(out, (h + e + 4, h - e + 4, h + 2)):
        one_copy.wait_recv()
        net.share_cat(block(lax.rem(key, 4)))


def all_of_8(block, whole, k, targets, net):
    out = [net.copy(block(k), block(k), to) for to in targets]
    yield
    for one_copy in out:
        one_copy.wait_recv()
    net.share(whole)


def ring_of_4(block, x, c, up, down, share, net):
    a = net.copy(block(x), block(x), up)
    b = net.copy(block(x), block(x), down)
    yield
    a.wait_recv()
    b.wait_recv()
    key = lax.rem(x + 3 + 2 * c, 4)
    to = {n: jnp.where(c == 0, up[n], down[n]) for n in up}
    a = net.copy(block(key), block(key), to)
    share(block(lax.rem(x + 3, 4)))
    share(block(lax.rem(x + 1, 4)))
    yield
    a.wait_recv()
    share(block(lax.rem(x + 2, 4)))


def flows_of(net, g, catb, wb):
    a = net.at
    x, yl, c, z, yh, zh, y = a["x"], a["yl"], a["c"], a["z"], a["yh"], g["zh"], g["y"]
    t_a, t_b, t_c = 4 * c, 4 * c + 1, pl.ds(4 * c + 2, 2)

    def w_a():
        yield from all_of_8(lambda k: wb.at[t_a, :, z, k], wb.at[t_a, :, z], y, g["ys"], net)
        yield from ring_of_8(lambda k: wb.at[t_a, :, k], z, c, g["z_up"], g["z_down"], net)

    def w_b():
        yield from all_of_8(lambda k: wb.at[t_b, :, k, y], wb.at[t_b, :, :, y], z, g["zs"], net)
        yield from ring_of_8(lambda k: wb.at[t_b, :, :, k], y, c, g["y_up"], g["y_down"], net)

    def quarter(of, zs, ys):
        rows = pl.ds(pl.multiple_of(8 * (of // 2), 8), 8)
        return wb.at[4 * c + 2 + lax.rem(of, 2), :, zs, ys, rows]

    def w_c():
        every = pl.ds(0, 8)
        yield from all_of_8(lambda k: quarter(x, z, k), quarter(x, z, every), y, g["ys"], net)
        ring = ring_of_8(lambda k: quarter(x, k, every), z, c, g["z_up"], g["z_down"], net)
        across = []
        for keys in ((0,), (7, 1), (6, 2), (5, 3), (4,)):
            more = next(ring, 0) is None
            for f in list(across):
                if next(f, 0) == 0:
                    across.remove(f)
            for k in keys:
                key = lax.rem(z + k, 8)
                f = ring_of_4(lambda of, key=key: quarter(of, key, every), x, c, g["xs"][0], g["xs"][1], net.share, net)
                next(f)
                across.append(f)
            yield
        while across:
            for f in list(across):
                if next(f, 0) == 0:
                    across.remove(f)
            yield

    def swap_y(first, second, both):
        one_copy = net.copy(first, first, g["y_far"])
        two = net.copy(second, second, g["y_near"])
        yield
        one_copy.wait_recv()
        two.wait_recv()
        net.share_cat(both)

    def cat_ab():
        net.share_cat(catb.at[pl.ds(4 * c, 4), x, yl, :, zh])
        ref = catb.at[pl.ds(4 * c, 2), x, yl, :, zh]
        out = [net.copy(ref, ref, to) for to in g["xs"]]
        yield
        for one_copy, s in zip(out, (1, 3, 2)):
            one_copy.wait_recv()
            net.share_cat(catb.at[pl.ds(4 * c, 2), lax.rem(x - s + 4, 4), yl, :, zh])
        both = [cat_a(), cat_b()]
        while both:
            tick(both)
            yield

    def cat_a():
        yield from swap_y(catb.at[t_a, pl.ds(0, 2), yl, :, zh], catb.at[t_a, pl.ds(2, 2), yl, :, zh],
                          catb.at[t_a, :, 1 - yl, :, zh])
        yield from pair_ring(lambda h: catb.at[t_a, :, :, :, h], zh, g["e"], 4, g["z_far"], g["z_near"], net)

    def cat_b():
        yield from pair_run(lambda h: catb.at[t_b, :, yl, :, h], zh, g["e"], g["z_run"], net)
        yield from swap_y(catb.at[t_b, pl.ds(0, 2), yl], catb.at[t_b, pl.ds(2, 2), yl], catb.at[t_b, :, 1 - yl])

    def cat_c():
        yield from pair_run(lambda h: catb.at[t_c, x, yl, :, h], zh, g["e"], g["z_run"], net)
        yield from swap_y(catb.at[t_c, x, yl, 0], catb.at[t_c, x, yl, 1], catb.at[t_c, x, 1 - yl])
        yield from ring_of_4(lambda k: catb.at[t_c, k], x, c, g["xs"][0], g["xs"][1], net.share_cat, net)

    return [cat_c(), cat_ab()], [w_c(), w_a(), w_b()]


def tick(flows):
    for f in list(flows):
        try:
            next(f)
        except StopIteration:
            flows.remove(f)


def layer(len_hbm, ids_hbm, tl_hbm, taps_hbm, gains_hbm, cat_hbm, gate_hbm, up_hbm, down_hbm, out_ref,
          lens, ids, tl, taps, gains, pair, pairs, catb, wb, hr, ht, h, keep, first, live, hid, nf, nt, far, inner, act,
          load_sem, fill_sem, send, recv):
    net = Net(send, recv)
    g = geometry(net)
    a = net.at
    x, yl, c, z, yh, zh, y = a["x"], a["yl"], a["c"], a["z"], a["yh"], g["zh"], g["y"]
    loads = []
    for n, (src, dst) in enumerate(((cat_hbm, pair), (ids_hbm, ids.at[1]), (len_hbm, lens), (tl_hbm, tl), (gains_hbm, gains), (taps_hbm, taps))):
        loads.append(pltpu.make_async_copy(src, dst, load_sem.at[n]))
        loads[-1].start()
    fill = []
    mine = pl.ds(pl.multiple_of(16 * yl, 16), 16)
    part = pl.ds(pl.multiple_of(8 * (x // 2), 8), 8)
    mine_part = pl.ds(pl.multiple_of(16 * yl + 8 * (x // 2), 8), 8)
    third = 2 + lax.rem(x, 2)
    for n, ref in enumerate((gate_hbm, up_hbm, down_hbm)):
        for t in range(3):
            if t < 2:
                src = ref.at[mine, pl.ds(pl.multiple_of(512 * c + 128 * t, 128), 128)]
                dst = wb.at[4 * c + t, n, z, y]
            else:
                src = ref.at[mine_part, pl.ds(pl.multiple_of(512 * c + 128 * third, 128), 128)]
                dst = wb.at[4 * c + third, n, z, y, part]
            fill.append(pltpu.make_async_copy(src, dst, fill_sem.at[3 * n + t]))
            fill[-1].start()
    near = entry_signals(g)
    loads[2].wait()
    base = jnp.int32(0)
    for n, size in SIZES:
        base = base * size + a[n]
    base = base * 256
    for k in (0, 1, 3, 4, 5):
        loads[k].wait()
    for one_copy in fill:
        one_copy.wait()
    pl.semaphore_wait(pltpu.get_barrier_semaphore(), near)

    shared, shared_cat = [], []
    net.share = lambda ref: shared.append(net.copy(ref, ref, g["twin"]))
    net.share_cat = lambda ref: shared_cat.append(net.copy(ref, ref, g["twin"]))
    cats, weights = flows_of(net, g, catb, wb)
    slot = 4 * lax.rem(z, 2) + yh
    group = []
    for to in g["group"]:
        half = pl.ds(pl.multiple_of(512 * to["c"], 512), 512)
        group.append(net.copy(pair.at[:, half], pairs.at[c, slot], to))
    before = net.copy(ids.at[1], ids.at[0], g["next"])
    pairs[c, slot] = jnp.where(c == 0, pair[:, 0:512], pair[:, 512:1024])
    tick(weights)
    user_tables(base, lens, keep, first, live)
    tap_rows(tl, taps, hr)
    tap_shifts(hr, ht, 0, 3)
    for one_copy in group:
        one_copy.wait_recv()
    for k in range(2):
        rows = jnp.concatenate([pairs[k, i].astype(F32) for i in range(8)], axis=0).astype(BF)
        for t in range(4):
            catb[4 * c + t, x, yl, k, zh] = rows[:, 128 * t:128 * t + 128]
    tick(cats)
    tick(weights)
    tap_shifts(hr, ht, 3, 5)
    tick(cats)
    tap_shifts(hr, ht, 8, 5)
    tick(cats)
    tick(weights)
    tap_shifts(hr, ht, 13, 3)
    tap_flips(ht, h, 0, 4)
    tick(cats)
    tick(weights)
    tap_flips(ht, h, 4, 6)
    tick(cats)
    tick(weights)
    tap_flips(ht, h, 10, 6)
    while cats:
        tick(cats)
    before.wait_recv()
    for one_copy in shared_cat:
        one_copy.wait_recv()
    look_up(ids, catb, gains, hid, nf, nt)
    tick(weights)
    windows(nt, first, ht, 0, 16)
    for s in range(4):
        tick(weights)
        if s < 3:
            windows(nt, first, ht, 16 * s + 16, 16)
        near_taps(tl, taps, keep, nf, hid, (2 * s, 2 * s + 1))
        far_taps(ht, h, live, far, s)
    while weights:
        tick(weights)
    for one_copy in shared:
        one_copy.wait_recv()
    feed_forward(gains, wb, far, hid, inner, act, out_ref)
    net.finish()


def body(item_ids, user_lengths, catalogue, tap_lengths, conv_taps, norm_gains, gate_weight, up_weight, down_weight):
    anywhere = pl.BlockSpec(memory_space=pl.ANY)
    return pl.pallas_call(
        layer,
        out_shape=jax.ShapeDtypeStruct((256, 1024), BF),
        in_specs=[anywhere] * 9,
        out_specs=pl.BlockSpec(memory_space=pltpu.VMEM),
        scratch_shapes=[
            pltpu.SMEM((32,), jnp.int32),
            pltpu.VMEM((2, 1, 256), jnp.int32),
            pltpu.VMEM((1, 1024), jnp.int32),
            pltpu.VMEM((256, 1024), BF),
            pltpu.VMEM((2, 1024), F32),
            pltpu.VMEM((2, 1024), BF),
            pltpu.VMEM((2, 8, 2, 512), BF),
            pltpu.VMEM((8, 4, 2, 2, 4, 16, 128), BF),
            pltpu.VMEM((8, 3, 8, 8, 16, 128), BF),
            pltpu.VMEM((1024, 256), BF),
            pltpu.VMEM((64, 16, 16, 256), BF),
            pltpu.VMEM((64, 256, 256), BF),
            pltpu.VMEM((16, 256, 128), F32),
            pltpu.VMEM((16, 256), BF),
            pltpu.VMEM((256, 128), F32),
            pltpu.VMEM((256, 1024), F32),
            pltpu.VMEM((272, 1024), F32),
            pltpu.VMEM((1024, 512), BF),
            pltpu.VMEM((4, 256, 256), F32),
            pltpu.VMEM((256, 1024), BF),
            pltpu.VMEM((256, 1024), BF),
            pltpu.SemaphoreType.DMA((6,)),
            pltpu.SemaphoreType.DMA((9,)),
            pltpu.SemaphoreType.DMA((N_SEM,)),
            pltpu.SemaphoreType.DMA((N_SEM,)),
        ],
        compiler_params=pltpu.CompilerParams(
            collective_id=0, has_side_effects=True, vmem_limit_bytes=66_000_000),
    )(user_lengths, item_ids.reshape(1, 256), tap_lengths, conv_taps[0], norm_gains[0], catalogue,
      gate_weight[0], up_weight[0], down_weight[0])


def solution(mesh):
    finer = Mesh(mesh.devices.reshape([size for _, size in SIZES]), [name for name, _ in SIZES])
    every, col = ("x", "yl", "c", "z", "yh"), ("z", "yh")
    placed = (P(every), P(), P(every, None), P(), P(), P(), P(None, col, None), P(None, col, None), P(None, col, None))
    return jax.shard_map(body, mesh=finer, in_specs=placed, out_specs=P(every, None), check_vma=False)
```
